1024 devices in a mesh: dp: 8 (over z_lo), blk: 16 (over y, core), aa: 8 (over z_hi, x).
Axes of the slice: x: 4, y: 8, z: 16 (z_hi: 2, z_lo: 8; z = z_hi * 8 + z_lo), core: 2. Of those that a mesh axis runs over, the one named last changes fastest.
Arguments:
- queries: bfloat16 [8, 16384, 2048], P('dp', ('blk', 'aa')), may hold values from -128 to 128
- keys: bfloat16 [8, 16384, 512], P('dp', ('blk', 'aa')), may hold values from -10 to 10
- values: bfloat16 [8, 16384, 512], P('dp', ('blk', 'aa')), may hold values from -6 to 6
- grad_parts: float32 [8, 128, 131072], P('dp', ('blk', 'aa')), may hold values from -768 to 768
Outputs:
- attended: bfloat16 [8, 16384, 2048], P('dp', 'blk', 'aa')
- grad_mean: float32 [131072], P(('blk', 'aa'))
The draws below stay inside these ranges and needn't reach their ends.
All inputs are finite; a program needn't handle non-finite values.
Results may differ from the reference program's by a relative error of at most 0.008.
Values may be sent and summed in bfloat16 or wider, within the bound.
No kernel may reach another device: no remote copies, remote signals or barrier semaphores. Data moves between devices by JAX's collectives and lax.ppermute only.
A program may use at most 32 MiB of HBM per device.

```python
import jax
import jax.numpy as jnp
from jax import lax

HQ = 16
KVH = 4
DH = 128
TOK_DEV = 128
BUCKET = 131072
SEQ = 16384
N_DP = 8
N_BLK = 16
N_AA = 8


def draw_keys(key, part):
    total_rows = TOK_DEV * N_BLK * N_AA
    drawn = jnp.clip(jax.random.normal(jax.random.fold_in(key, 21), (N_DP, total_rows, KVH * DH), jnp.float32), -6.0, 6.0)
    return drawn.astype(jnp.bfloat16)


def draw_queries(key, part):
    total_rows = TOK_DEV * N_BLK * N_AA
    drawn = jnp.clip(jax.random.normal(jax.random.fold_in(key, 31), (N_DP, total_rows, HQ * DH), jnp.float32), -6.0, 6.0)
    return drawn.astype(jnp.bfloat16)


def raised(drawn, key, source, target, shards_of, factor):
    def block_of(dim):
        return (jnp.arange(drawn.shape[dim]) // (drawn.shape[dim] // shards_of)).reshape((-1,) + (1,) * (drawn.ndim - 1 - dim))

    first = jax.random.permutation(key, shards_of)[block_of(target)]
    other_side = (block_of(target) + shards_of // 2) % shards_of
    return jnp.where((block_of(source) == first) | (block_of(source) == other_side), factor * drawn, drawn)


def level_of(own_key, dims, shards, least, largest):
    gain, own = 1.0, jax.random.fold_in(own_key, 6)
    for axis_at, parts in shards:
        draws = jnp.exp(jax.random.uniform(jax.random.fold_in(own, axis_at), (parts,), jnp.float32, least / len(shards), largest / len(shards)))
        gain = gain * jnp.repeat(draws, dims[axis_at] // parts).reshape([-1 if axis == axis_at else 1 for axis in range(len(dims))])
    return gain


def centred(key, extent, deviation, bound, cuts=(), held_as=jnp.bfloat16):
    factor_of = level_of(key, extent, cuts, -0.22, 0.18) if cuts else 1.0
    entries = jax.random.normal(key, extent, jnp.float32) * deviation * factor_of
    return jnp.minimum(jnp.maximum(entries, -bound), bound).astype(held_as)


def heavy_noise(key, dims, scale, most, shards, heavy, held_as=jnp.bfloat16):
    array = scale * jax.random.normal(key, dims, jnp.float32)
    if shards:
        array = array * level_of(key, dims, shards, -0.22, 0.18)
    return jnp.clip(raised(array, jax.random.fold_in(key, 3), *heavy), -most, most).astype(held_as)


def setup_inputs(seed: int = 0) -> dict:
    seeds = jax.random.split(jax.random.key(seed), 5)
    return {
        "queries": draw_queries(jax.random.fold_in(seeds[4], 71), 0),
        "keys": draw_keys(jax.random.fold_in(seeds[4], 71), 0),
        "values": centred(seeds[2], (N_DP, SEQ, KVH * DH), 1.0, 6.0, ((0, 8), (1, 128))),
        "grad_parts": heavy_noise(seeds[3], (N_DP, N_BLK * N_AA, BUCKET), 32.0, 768.0, ((0, 8), (1, 128)), (1, 2, 128, 5.5), jnp.float32),
    }


def attend_one(q_rep, k_rep, v_rep):
    total_rows = q_rep.shape[0]
    reach = total_rows // (4 * N_BLK)
    step_rows = min(256, reach)
    group = HQ // KVH
    q_heads = q_rep.reshape(total_rows, HQ, DH)
    pad_zero = jnp.zeros((reach, KVH, DH), jnp.bfloat16)
    k_padded = jnp.concatenate([pad_zero, k_rep.reshape(total_rows, KVH, DH)], 0)
    v_padded = jnp.concatenate([pad_zero, v_rep.reshape(total_rows, KVH, DH)], 0)
    scale = DH ** -0.5

    def one_block(index):
        start = (index * step_rows).astype(jnp.int32)
        q_block = lax.dynamic_slice_in_dim(q_heads, start, step_rows, 0).astype(jnp.float32)
        k_block = jnp.repeat(lax.dynamic_slice_in_dim(k_padded, start, step_rows + reach, 0), group, axis=1).astype(jnp.float32)
        v_block = jnp.repeat(lax.dynamic_slice_in_dim(v_padded, start, step_rows + reach, 0), group, axis=1).astype(jnp.float32)
        scores = jnp.einsum("qhd,khd->hqk", q_block, k_block) * scale
        q_pos = start + jnp.arange(step_rows, dtype=jnp.int32)
        k_pos = start - reach + jnp.arange(step_rows + reach, dtype=jnp.int32)
        allowed = (k_pos[None, :] <= q_pos[:, None]) & (k_pos[None, :] > q_pos[:, None] - reach)
        scores = jnp.where(allowed[None], scores, -1e30)
        top = jnp.max(scores, axis=-1, keepdims=True)
        expo = jnp.exp(scores - top)
        weights = (expo / jnp.sum(expo, axis=-1, keepdims=True)).astype(jnp.bfloat16)
        out = jnp.einsum("hqk,khd->qhd", weights.astype(jnp.float32), v_block)
        return out.astype(jnp.bfloat16)

    blocks = lax.map(one_block, jnp.arange(total_rows // step_rows, dtype=jnp.int32))
    return blocks.reshape(total_rows, HQ * DH)


def reference(queries, keys, values, grad_parts):
    def one_replica(triple):
        return attend_one(triple[0], triple[1], triple[2])

    attended = lax.map(one_replica, (queries, keys, values))
    count = grad_parts.shape[0] * grad_parts.shape[1]
    grad_mean = jnp.sum(grad_parts.astype(jnp.float32), axis=(0, 1)) / count
    return attended, grad_mean
```

```python
import jax
import jax.numpy as jnp
from jax import lax
from jax.experimental import pallas as pl
from jax.experimental.pallas import tpu as pltpu
from jax.sharding import Mesh
from jax.sharding import PartitionSpec as P

DH = 128
BLK = ("blk_0", "blk_1")
AA = ("aa_0", "aa_1")
BLK_AA = ("blk_0", "blk_1", "aa_0", "aa_1")
SWAP = [(0, 1), (1, 0)]


def pack_kernel(side_ref, q_ref, k_ref, v_ref, far_q, far_kv, near):
    side = side_ref[0]
    n, _, wide = far_q.shape
    for x in range(n):
        for half, is_far in ((1 - side, True), (side, False)):
            q_at = pl.multiple_of(half * (n * wide) + x * wide, wide)
            q_part = q_ref[:, pl.ds(q_at, wide)]
            kv_at = pl.multiple_of(half * (n // 2 * DH) + x // 2 * DH, DH)
            k_part = k_ref[:, pl.ds(kv_at, DH)]
            v_part = v_ref[:, pl.ds(kv_at, DH)]
            if is_far:
                far_q[x] = q_part
                if x % 2 == 0:
                    far_kv[x // 2, :, :DH] = k_part
                    far_kv[x // 2, :, DH:] = v_part
            else:
                near[x, :, :wide] = q_part
                near[x, :, wide : wide + DH] = k_part
                near[x, :, wide + DH :] = v_part


def packed(side, q, k, v, n):
    rows, wide = q.shape[0], q.shape[1] // (2 * n)
    vmem = pl.BlockSpec(memory_space=pltpu.VMEM)
    return pl.pallas_call(
        pack_kernel,
        out_shape=(
            jax.ShapeDtypeStruct((n, rows, wide), q.dtype),
            jax.ShapeDtypeStruct((n // 2, rows, 2 * DH), q.dtype),
            jax.ShapeDtypeStruct((n, rows, wide + 2 * DH), q.dtype),
        ),
        in_specs=[pl.BlockSpec(memory_space=pltpu.SMEM), vmem, vmem, vmem],
        out_specs=(vmem, vmem, vmem),
        compiler_params=pltpu.CompilerParams(vmem_limit_bytes=8 << 20),
        name="pack",
    )(side, q, k, v)


def attend_kernel(side_ref, near_ref, far_kv_ref, far_q_ref, prior_ref, out_ref, q_s, k_s, v_s):
    side = side_ref[0]
    half, wide = far_q_ref.shape
    reach = prior_ref.shape[0]
    near_at = pl.multiple_of(side * half, half)
    far_at = pl.multiple_of((1 - side) * half, half)
    k_s[:reach] = prior_ref[:, :DH]
    v_s[:reach] = prior_ref[:, DH:]
    for at, kv in ((near_at, near_ref[:, wide:]), (far_at, far_kv_ref[...])):
        k_s[pl.ds(at + reach, half)] = kv[:, :DH]
        v_s[pl.ds(at + reach, half)] = kv[:, DH:]
    q_s[pl.ds(near_at, half)] = near_ref[:, :wide]
    q_s[pl.ds(far_at, half)] = far_q_ref[...]
    row = lax.broadcasted_iota(jnp.int32, (reach, reach), 0)
    col = lax.broadcasted_iota(jnp.int32, (reach, reach), 1)
    newer = col <= row
    across = (((1,), (1,)), ((), ()))
    for block in range(2 * half // reach):
        rows = pl.ds(block * reach, reach)
        older_rows, newer_rows = rows, pl.ds((block + 1) * reach, reach)
        for head in range(wide // DH):
            lanes = pl.ds(head * DH, DH)
            q = q_s[rows, lanes]
            old = lax.dot_general(q, k_s[older_rows], across, preferred_element_type=jnp.float32)
            new = lax.dot_general(q, k_s[newer_rows], across, preferred_element_type=jnp.float32)
            scores = jnp.where(newer, new, old) * DH**-0.5
            expo = jnp.exp(scores - jnp.max(scores, axis=-1, keepdims=True))
            weights = (expo / jnp.sum(expo, axis=-1, keepdims=True)).astype(jnp.bfloat16)
            none = jnp.zeros_like(weights)
            out = jnp.dot(
                jnp.where(newer, weights, none), v_s[newer_rows], preferred_element_type=jnp.float32
            ) + jnp.dot(
                jnp.where(newer, none, weights), v_s[older_rows], preferred_element_type=jnp.float32
            )
            out_ref[rows, lanes] = out.astype(jnp.bfloat16)


def attended_rows(side, near, far_kv, far_q, prior):
    half, wide = far_q.shape
    reach = prior.shape[0]
    vmem = pl.BlockSpec(memory_space=pltpu.VMEM)
    return pl.pallas_call(
        attend_kernel,
        out_shape=jax.ShapeDtypeStruct((2 * half, wide), jnp.bfloat16),
        in_specs=[pl.BlockSpec(memory_space=pltpu.SMEM), vmem, vmem, vmem, vmem],
        out_specs=vmem,
        scratch_shapes=[
            pltpu.VMEM((2 * half, wide), jnp.bfloat16),
            pltpu.VMEM((2 * half + reach, DH), jnp.bfloat16),
            pltpu.VMEM((2 * half + reach, DH), jnp.bfloat16),
        ],
        cost_estimate=pl.CostEstimate(
            flops=16 * half * wide * reach, bytes_accessed=4 * half * wide * 2, transcendentals=4 * half * reach
        ),
        compiler_params=pltpu.CompilerParams(vmem_limit_bytes=16 << 20),
        name="attend",
    )(side, near, far_kv, far_q, prior)


def step(queries, keys, values, grad_parts):
    n = lax.axis_size("aa_1")
    side = lax.axis_index("aa_0").astype(jnp.int32)
    side_at = side.reshape(1)
    far_q, far_kv, near = packed(side_at, queries[0], keys[0], values[0], n)
    far_kv = lax.ppermute(far_kv, "aa_0", SWAP)
    far_q = lax.ppermute(far_q, "aa_0", SWAP)
    near = lax.all_to_all(near, "aa_1", 0, 0, tiled=True)
    near = near.reshape(-1, near.shape[-1])

    dp, y, c, z, x = (lax.axis_size(a) for a in ("dp", *BLK_AA))
    parts = grad_parts.reshape(y * c, z, x, 1, -1).transpose(0, 2, 1, 3, 4)
    parts = parts.reshape(y * c * x, 1, -1)
    parts = lax.all_to_all(parts, ("blk_0", "blk_1", "aa_1"), 0, 0, tiled=True)
    share = jnp.sum(parts, axis=0).reshape(z, 1, -1)
    share = jnp.broadcast_to(share[None], (dp, *share.shape)).reshape(dp * z, 1, -1)
    share = lax.all_to_all(share, ("dp", "aa_0"), 0, 0, tiled=True)
    grad_mean = jnp.sum(share, axis=(0, 1)) / (dp * y * c * z * x)

    far_kv = lax.all_to_all(jnp.repeat(far_kv, 2, axis=0), "aa_1", 0, 0, tiled=True)
    far_kv = far_kv.reshape(-1, far_kv.shape[-1])
    half = near.shape[0]
    reach = half // 2
    last = jnp.where(side == 1, near[half - reach :, -2 * DH :], far_kv[half - reach :])
    prior = lax.ppermute(last, BLK, [(i, i + 1) for i in range(y * c - 1)])
    far_q = lax.all_to_all(far_q, "aa_1", 0, 0, tiled=True)
    far_q = far_q.reshape(-1, far_q.shape[-1])
    attended = attended_rows(side_at, near, far_kv, far_q, prior)
    return attended[None], grad_mean


def solution(mesh):
    torus = Mesh(
        mesh.devices.reshape(mesh.shape["dp"], 8, 2, 2, 4), ("dp", "blk_0", "blk_1", "aa_0", "aa_1")
    )
    placed = P("dp", BLK_AA, None)
    return jax.shard_map(
        step,
        mesh=torus,
        in_specs=(placed,) * 4,
        out_specs=(P("dp", BLK, AA), P(BLK_AA)),
        check_vma=False,
    )
```

```python
import jax
import jax.numpy as jnp
from jax import lax
from jax.experimental import pallas as pl
from jax.experimental.pallas import tpu as pltpu
from jax.sharding import Mesh
from jax.sharding import PartitionSpec as P

DH = 128
BLK = ("blk_0", "blk_1")
AA = ("aa_0", "aa_1")
BLK_AA = ("blk_0", "blk_1", "aa_0", "aa_1")


def place(at_ref, n):
    at = at_ref[0]
    return lax.div(at, n), lax.rem(at, n)


def pack_kernel(n, at_ref, q_ref, k_ref, v_ref, g_ref, *refs):
    kv_to, q_to, near_to, g_to, sems = refs[:2], refs[2 : 2 + n], refs[2 + n : 2 + 2 * n], refs[-2], refs[-1]
    side, x = place(at_ref, n)
    wide = q_to[0].shape[1]
    moves = []

    def lanes(ref, index, width):
        return ref.at[:, pl.ds(pl.multiple_of(index * width, width), width)]

    def kv_move(head, to, at):
        moves.append((lanes(k_ref, head, DH), to.at[:, at : at + DH]))
        moves.append((lanes(v_ref, head, DH), to.at[:, at + DH : at + 2 * DH]))

    for hop, to in zip((0, n // 2), kv_to):
        kv_move((1 - side) * (n // 2) + lax.div(lax.rem(x + hop, n), 2), to, 0)
    for hop in range(n):
        target = lax.rem(x + hop, n)
        moves.append((lanes(q_ref, (1 - side) * n + target, wide), q_to[hop]))
        moves.append((lanes(q_ref, side * n + target, wide), near_to[hop].at[:, :wide]))
        kv_move(side * (n // 2) + lax.div(target, 2), near_to[hop], wide)
    chunk = g_ref.shape[-1]
    for z in range(g_ref.shape[1]):
        moves.append((g_ref.at[:, z], g_to.at[:, :, :, z * chunk : (z + 1) * chunk]))
    copies = [pltpu.make_async_copy(a, b, sems.at[i]) for i, (a, b) in enumerate(moves)]
    for copy in copies:
        copy.start()
    for copy in copies:
        copy.wait()


def packed(at, q, k, v, g, n):
    rows, wide = q.shape[0], q.shape[1] // (2 * n)
    vmem = pl.BlockSpec(memory_space=pltpu.VMEM)
    hbm = pl.BlockSpec(memory_space=pltpu.HBM)
    piece = jax.ShapeDtypeStruct((rows, wide), q.dtype)
    near = jax.ShapeDtypeStruct((rows, wide + 2 * DH), q.dtype)
    yc, z, x, _, chunk = g.shape
    outs = (
        *(jax.ShapeDtypeStruct((rows, 2 * DH), q.dtype),) * 2,
        *(piece,) * n,
        *(near,) * n,
        jax.ShapeDtypeStruct((yc, x, 1, z * chunk), g.dtype),
    )
    found = pl.pallas_call(
        lambda *refs: pack_kernel(n, *refs),
        out_shape=outs,
        in_specs=[pl.BlockSpec(memory_space=pltpu.SMEM), hbm, hbm, hbm, hbm],
        out_specs=(vmem,) * len(outs),
        scratch_shapes=[pltpu.SemaphoreType.DMA((4 + 4 * n + z,))],
        compiler_params=pltpu.CompilerParams(vmem_limit_bytes=8 << 20),
        name="pack",
    )(at, q, k, v, g)
    return found[:2], found[2 : 2 + n], found[2 + n : 2 + 2 * n], found[-1]


def gather_kernel(n, at_ref, *refs):
    near, own, swapped, (kv_ref, last_ref) = refs[:n], refs[n : n + 2], refs[n + 2], refs[n + 3 :]
    side, x = place(at_ref, n)
    rows, width = own[0].shape

    def put(half, chunk, value):
        kv_ref[pl.ds(pl.multiple_of((half * n + chunk) * rows, rows), rows)] = value

    for hop in range(n):
        put(side, lax.rem(x + n - hop, n), near[hop][:, -width:])
    mate = x + 1 - 2 * lax.rem(x, 2)
    for i, hop in enumerate((0, n // 2)):
        put(1 - side, lax.rem(x + hop, n), own[i][...])
        put(1 - side, lax.rem(mate + hop, n), swapped[i])
    last_ref[...] = kv_ref[kv_ref.shape[0] - last_ref.shape[0] :]


def gathered(at, near, own, swapped, reach):
    n = len(near)
    rows, width = own[0].shape
    vmem = pl.BlockSpec(memory_space=pltpu.VMEM)
    return pl.pallas_call(
        lambda *refs: gather_kernel(n, *refs),
        out_shape=(
            jax.ShapeDtypeStruct((2 * n * rows, width), jnp.bfloat16),
            jax.ShapeDtypeStruct((reach, width), jnp.bfloat16),
        ),
        in_specs=[pl.BlockSpec(memory_space=pltpu.SMEM)] + [vmem] * (n + 3),
        out_specs=(vmem, vmem),
        compiler_params=pltpu.CompilerParams(vmem_limit_bytes=8 << 20),
        name="gather",
    )(at, *near, *own, swapped)


def attend_kernel(n, at_ref, kv_ref, prior_ref, *refs):
    near, far, out_ref, q_s = refs[:n], refs[n : 2 * n], refs[2 * n], refs[2 * n + 1]
    side, x = place(at_ref, n)
    rows, wide = far[0].shape
    reach = prior_ref.shape[0]
    for hop in range(n):
        chunk = lax.rem(x + n - hop, n)
        q_s[pl.ds(pl.multiple_of((side * n + chunk) * rows, rows), rows)] = near[hop][:, :wide]
        q_s[pl.ds(pl.multiple_of(((1 - side) * n + chunk) * rows, rows), rows)] = far[hop][...]
    row = lax.broadcasted_iota(jnp.int32, (reach, reach), 0)
    col = lax.broadcasted_iota(jnp.int32, (reach, reach), 1)
    newer = col <= row
    across = (((1,), (1,)), ((), ()))
    for block in range(2 * n * rows // reach):
        here = pl.ds(block * reach, reach)
        older_ref, older = (kv_ref, pl.ds((block - 1) * reach, reach)) if block else (prior_ref, slice(None))
        for head in range(wide // DH):
            lanes = pl.ds(head * DH, DH)
            q = q_s[here, lanes]
            old = lax.dot_general(q, older_ref[older, :DH], across, preferred_element_type=jnp.float32)
            new = lax.dot_general(q, kv_ref[here, :DH], across, preferred_element_type=jnp.float32)
            scores = jnp.where(newer, new, old) * DH**-0.5
            expo = jnp.exp(scores - jnp.max(scores, axis=-1, keepdims=True))
            weights = (expo / jnp.sum(expo, axis=-1, keepdims=True)).astype(jnp.bfloat16)
            none = jnp.zeros_like(weights)
            out = jnp.dot(
                jnp.where(newer, weights, none), kv_ref[here, DH:], preferred_element_type=jnp.float32
            ) + jnp.dot(
                jnp.where(newer, none, weights), older_ref[older, DH:], preferred_element_type=jnp.float32
            )
            out_ref[here, lanes] = out.astype(jnp.bfloat16)


def attended_rows(at, kv, prior, near, far):
    n = len(near)
    wide, reach = far[0].shape[1], prior.shape[0]
    vmem = pl.BlockSpec(memory_space=pltpu.VMEM)
    total = kv.shape[0]
    return pl.pallas_call(
        lambda *refs: attend_kernel(n, *refs),
        out_shape=jax.ShapeDtypeStruct((total, wide), jnp.bfloat16),
        in_specs=[pl.BlockSpec(memory_space=pltpu.SMEM)] + [vmem] * (2 + 2 * n),
        out_specs=vmem,
        scratch_shapes=[pltpu.VMEM((total, wide), jnp.bfloat16)],
        cost_estimate=pl.CostEstimate(
            flops=8 * total * wide * reach, bytes_accessed=4 * total * wide * 2, transcendentals=2 * total * reach
        ),
        compiler_params=pltpu.CompilerParams(vmem_limit_bytes=16 << 20),
        name="attend",
    )(at, kv, prior, *near, *far)


def step(queries, keys, values, grad_parts):
    dp, y, c, z, n = (lax.axis_size(a) for a in ("dp", *BLK_AA))
    at = lax.axis_index(AA).astype(jnp.int32).reshape(1)
    chunks = grad_parts.reshape(y * c, z, n, 1, -1)
    kv_far, q_far, near, parts = packed(at, queries[0], keys[0], values[0], chunks, n)

    def hopped(value, hop, across):
        pairs = [
            (s * n + x, (1 - s if across else s) * n + (x + hop) % n) for s in range(z) for x in range(n)
        ]
        return lax.ppermute(value, AA, pairs)

    own = [hopped(kv_far[i], hop, True) for i, hop in enumerate((0, n // 2))]
    far = [hopped(q_far[hop], hop, True) for hop in range(n)]
    parts = parts.reshape(y * c * n, 1, -1)
    parts = lax.all_to_all(parts, ("blk_0", "blk_1", "aa_1"), 0, 0, tiled=True)
    near = [near[0]] + [hopped(near[hop], hop, False) for hop in range(1, n)]
    pairs = [(x, x ^ 1) for x in range(n)]
    swapped = lax.ppermute(jnp.stack(own), "aa_1", pairs)
    reach = queries.shape[1] * 2
    kv, last = gathered(at, near, own, swapped, reach)
    prior = lax.ppermute(last, BLK, [(i, i + 1) for i in range(y * c - 1)])

    share = jnp.sum(parts, axis=0).reshape(z, 1, -1)
    share = jnp.broadcast_to(share[None], (dp, *share.shape)).reshape(dp * z, 1, -1)
    share = lax.all_to_all(share, ("dp", "aa_0"), 0, 0, tiled=True)
    grad_mean = jnp.sum(share, axis=(0, 1)) / (dp * y * c * z * n)

    attended = attended_rows(at, kv, prior, near, far)
    return attended[None], grad_mean


def solution(mesh):
    torus = Mesh(
        mesh.devices.reshape(mesh.shape["dp"], 8, 2, 2, 4), ("dp", "blk_0", "blk_1", "aa_0", "aa_1")
    )
    placed = P("dp", BLK_AA, None)
    return jax.shard_map(
        step,
        mesh=torus,
        in_specs=(placed,) * 4,
        out_specs=(P("dp", BLK, AA), P(BLK_AA)),
        check_vma=False,
    )
```

```python
import jax
import jax.numpy as jnp
from jax import lax
from jax.experimental import pallas as pl
from jax.experimental.pallas import tpu as pltpu
from jax.sharding import Mesh
from jax.sharding import PartitionSpec as P

DH = 128
BLK = ("blk_0", "blk_1")
AA = ("aa_0", "aa_1")
BLK_AA = ("blk_0", "blk_1", "aa_0", "aa_1")


def place(at_ref, n):
    at = at_ref[0]
    return lax.div(at, n), lax.rem(at, n)


def place(at_ref, n):
    at = at_ref[0]
    return lax.div(at, n), lax.rem(at, n)


def run_all(moves, sems):
    copies = [pltpu.make_async_copy(a, b, sems.at[i]) for i, (a, b) in enumerate(moves)]
    for copy in copies:
        copy.start()
    for copy in copies:
        copy.wait()


def lanes_of(ref, index, width):
    return ref.at[:, pl.ds(pl.multiple_of(index * width, width), width)]


def pack_far_kernel(n, at_ref, k_ref, v_ref, kv_to, sems):
    side, _ = place(at_ref, n)
    moves = []
    for i in range(n // 2):
        head = (1 - side) * (n // 2) + i
        moves.append((lanes_of(k_ref, head, DH), kv_to.at[i, :, :DH]))
        moves.append((lanes_of(v_ref, head, DH), kv_to.at[i, :, DH:]))
    run_all(moves, sems)


def pack_kernel(n, at_ref, q_ref, k_ref, v_ref, g_ref, *refs):
    to, g_to, sems = refs[:n], refs[n], refs[n + 1]
    side, x = place(at_ref, n)
    wide = q_ref.shape[1] // (2 * n)
    moves = []
    chunk = g_ref.shape[-1]
    for z in range(g_ref.shape[1]):
        moves.append((g_ref.at[:, z], g_to.at[:, :, :, z * chunk : (z + 1) * chunk]))
    for hop in range(n):
        target = lax.rem(x + hop, n)
        head = side * (n // 2) + lax.div(target, 2)
        moves.append((lanes_of(q_ref, side * n + target, wide), to[hop].at[:, :wide]))
        moves.append((lanes_of(k_ref, head, DH), to[hop].at[:, wide : wide + DH]))
        moves.append((lanes_of(v_ref, head, DH), to[hop].at[:, wide + DH : wide + 2 * DH]))
        moves.append((lanes_of(q_ref, (1 - side) * n + target, wide), to[hop].at[:, wide + 2 * DH :]))
    run_all(moves, sems)


def kernel_call(body, outs, ins, name, scratch=(), limit=8 << 20, **more):
    vmem = pl.BlockSpec(memory_space=pltpu.VMEM)
    settings = dict(
        out_shape=outs,
        in_specs=[pl.BlockSpec(memory_space=pltpu.SMEM)] + [vmem] * (len(ins) - 1),
        out_specs=(vmem,) * len(outs),
        scratch_shapes=list(scratch),
        compiler_params=pltpu.CompilerParams(vmem_limit_bytes=limit),
        name=name,
    )
    settings.update(more)
    return pl.pallas_call(body, **settings)(*ins)


def packed_far(at, k, v, n):
    return kernel_call(
        lambda *refs: pack_far_kernel(n, *refs),
        (jax.ShapeDtypeStruct((n // 2, k.shape[0], 2 * DH), k.dtype),),
        (at, k, v),
        "pack_far",
        scratch=(pltpu.SemaphoreType.DMA((n,)),),
        in_specs=[pl.BlockSpec(memory_space=pltpu.SMEM)] + [pl.BlockSpec(memory_space=pl.ANY)] * 2,
    )[0]


def packed(at, q, k, v, g, n):
    rows, wide = q.shape[0], q.shape[1] // (2 * n)
    yc, z, x, _, chunk = g.shape
    outs = (
        *(jax.ShapeDtypeStruct((rows, 2 * wide + 2 * DH), q.dtype),) * n,
        jax.ShapeDtypeStruct((yc, x, 1, z * chunk), g.dtype),
    )
    found = kernel_call(
        lambda *refs: pack_kernel(n, *refs),
        outs,
        (at, q, k, v, g),
        "pack",
        scratch=(pltpu.SemaphoreType.DMA((4 * n + z,)),),
        in_specs=[pl.BlockSpec(memory_space=pltpu.SMEM)] + [pl.BlockSpec(memory_space=pl.ANY)] * 4,
    )
    return found[:n], found[-1]


def stack_kernel(n, *refs):
    for hop in range(n):
        refs[n][hop] = refs[hop][:, -refs[n].shape[-1] :]


def stacked(pieces, wide):
    n, rows = len(pieces), pieces[0].shape[0]
    vmem = pl.BlockSpec(memory_space=pltpu.VMEM)
    return kernel_call(
        lambda *refs: stack_kernel(n, *refs),
        (jax.ShapeDtypeStruct((n, rows, wide), pieces[0].dtype),),
        tuple(pieces),
        "stack",
        in_specs=[vmem] * n,
    )[0]


def cut_kernel(n, at_ref, kv_ref, *to):
    _, x = place(at_ref, n)
    for hop in range(n):
        to[hop][...] = kv_ref[lax.div(lax.rem(x + hop, n), 2)]


def cut(at, kv, n):
    outs = (jax.ShapeDtypeStruct(kv.shape[1:], kv.dtype),) * n
    return kernel_call(lambda *refs: cut_kernel(n, *refs), outs, (at, kv), "cut")


def gather_kernel(n, at_ref, *refs):
    near, far, (kv_ref, last_ref) = refs[:n], refs[n : 2 * n], refs[2 * n :]
    side, x = place(at_ref, n)
    rows, width = far[0].shape

    def put(half, chunk, value):
        kv_ref[pl.ds(pl.multiple_of((half * n + chunk) * rows, rows), rows)] = value

    for hop in range(n):
        chunk = lax.rem(x + n - hop, n)
        wide = (near[hop].shape[1] - width) // 2
        put(side, chunk, near[hop][:, wide : wide + width])
        put(1 - side, chunk, far[hop][...])
    last_ref[...] = kv_ref[kv_ref.shape[0] - last_ref.shape[0] :]


def gathered(at, near, far, reach):
    rows, width = far[0].shape
    n = len(near)
    outs = (
        jax.ShapeDtypeStruct((2 * n * rows, width), jnp.bfloat16),
        jax.ShapeDtypeStruct((reach, width), jnp.bfloat16),
    )
    return kernel_call(lambda *refs: gather_kernel(n, *refs), outs, (at, *near, *far), "gather")


def attend_kernel(n, is_near, count, at_ref, kv_ref, prior_ref, *refs):
    pieces, out_ref, q_s, older_s, out_s, sem = refs[:count], *refs[-5:]
    side, x = place(at_ref, n)
    half = side if is_near else 1 - side
    rows, wide = q_s.shape[0] // n, q_s.shape[1]
    reach = prior_ref.shape[0]
    for hop in range(n):
        chunk = lax.rem(x + n - hop, n)
        value = pieces[hop][:, :wide] if is_near else pieces[0][hop]
        q_s[pl.ds(pl.multiple_of(chunk * rows, rows), rows)] = value
    start = pl.multiple_of(half * n * rows, reach)

    @pl.when(half == 0)
    def _():
        older_s[...] = prior_ref[...]

    @pl.when(half != 0)
    def _():
        older_s[...] = kv_ref[n * rows - reach : n * rows]

    row = lax.broadcasted_iota(jnp.int32, (reach, reach), 0)
    col = lax.broadcasted_iota(jnp.int32, (reach, reach), 1)
    newer = col <= row
    across = (((1,), (1,)), ((), ()))
    for block in range(n * rows // reach):
        here = pl.ds(block * reach, reach)
        now = pl.ds(pl.multiple_of(start + block * reach, reach), reach)
        if block:
            older_ref, older = kv_ref, pl.ds(pl.multiple_of(start + (block - 1) * reach, reach), reach)
        else:
            older_ref, older = older_s, slice(None)
        for head in range(wide // DH):
            lanes = pl.ds(head * DH, DH)
            q = q_s[here, lanes]
            old = lax.dot_general(q, older_ref[older, :DH], across, preferred_element_type=jnp.float32)
            new = lax.dot_general(q, kv_ref[now, :DH], across, preferred_element_type=jnp.float32)
            scores = jnp.where(newer, new, old) * DH**-0.5
            expo = jnp.exp(scores - jnp.max(scores, axis=-1, keepdims=True))
            weights = (expo / jnp.sum(expo, axis=-1, keepdims=True)).astype(jnp.bfloat16)
            none = jnp.zeros_like(weights)
            out = jnp.dot(
                jnp.where(newer, weights, none), kv_ref[now, DH:], preferred_element_type=jnp.float32
            ) + jnp.dot(
                jnp.where(newer, none, weights), older_ref[older, DH:], preferred_element_type=jnp.float32
            )
            out_s[here, lanes] = out.astype(jnp.bfloat16)
    copy = pltpu.make_async_copy(out_s, out_ref.at[pl.ds(start, n * rows)], sem)
    copy.start()
    copy.wait()


def attended_half(at, kv, prior, pieces, n, wide, onto=None):
    reach, total = prior.shape[0], kv.shape[0]
    vmem, somewhere = pl.BlockSpec(memory_space=pltpu.VMEM), pl.BlockSpec(memory_space=pl.ANY)
    is_near = onto is None
    ins = (at, kv, prior, *pieces) + (() if is_near else (onto,))
    return kernel_call(
        lambda *refs: attend_kernel(n, is_near, len(pieces), *refs),
        (jax.ShapeDtypeStruct((total, wide), jnp.bfloat16),),
        ins,
        "attend",
        scratch=(
            pltpu.VMEM((total // 2, wide), jnp.bfloat16),
            pltpu.VMEM(prior.shape, jnp.bfloat16),
            pltpu.VMEM((total // 2, wide), jnp.bfloat16),
            pltpu.SemaphoreType.DMA,
        ),
        limit=16 << 20,
        in_specs=[pl.BlockSpec(memory_space=pltpu.SMEM)]
        + [vmem] * (2 + len(pieces))
        + ([] if is_near else [somewhere]),
        out_specs=(somewhere,),
        input_output_aliases={} if is_near else {3 + len(pieces): 0},
        cost_estimate=pl.CostEstimate(
            flops=4 * total * wide * reach, bytes_accessed=2 * total * wide * 2, transcendentals=total * reach
        ),
    )[0]


def step(queries, keys, values, grad_parts):
    dp, y, c, z, n = (lax.axis_size(a) for a in ("dp", *BLK_AA))
    at = lax.axis_index(AA).astype(jnp.int32).reshape(1)
    wide = queries.shape[2] // (z * n)
    reach = queries.shape[1] * 2
    chunks = grad_parts.reshape(y * c, z, n, 1, -1)
    kv_far = packed_far(at, keys[0], values[0], n)
    sent, parts = packed(at, queries[0], keys[0], values[0], chunks, n)

    def along_x(value, hop):
        return lax.ppermute(value, "aa_1", [(x, (x + hop) % n) for x in range(n)])

    def across_z(value):
        return lax.ppermute(value, "aa_0", [(s, 1 - s) for s in range(z)])

    kv_far = across_z(kv_far)
    parts = parts.reshape(y * c * n, 1, -1)
    parts = lax.all_to_all(parts, ("blk_0", "blk_1", "aa_1"), 0, 0, tiled=True)
    near = [sent[0]] + [along_x(sent[hop], hop) for hop in range(1, n)]
    q_far = stacked(near, wide)
    q_far = across_z(q_far)
    far = cut(at, kv_far, n)
    far = [far[0]] + [along_x(far[hop], hop) for hop in range(1, n)]
    kv, last = gathered(at, near, far, reach)
    prior = lax.ppermute(last, BLK, [(i, i + 1) for i in range(y * c - 1)])
    rows = attended_half(at, kv, prior, near, n, wide)

    share = jnp.sum(parts, axis=0).reshape(z, 1, -1)
    share = jnp.broadcast_to(share[None], (dp, *share.shape)).reshape(dp * z, 1, -1)
    share = lax.all_to_all(share, ("dp", "aa_0"), 0, 0, tiled=True)
    grad_mean = jnp.sum(share, axis=(0, 1)) / (dp * y * c * z * n)

    rows = attended_half(at, kv, prior, (q_far,), n, wide, rows)
    return rows[None], grad_mean


def solution(mesh):
    torus = Mesh(
        mesh.devices.reshape(mesh.shape["dp"], 8, 2, 2, 4), ("dp", "blk_0", "blk_1", "aa_0", "aa_1")
    )
    placed = P("dp", BLK_AA, None)
    return jax.shard_map(
        step,
        mesh=torus,
        in_specs=(placed,) * 4,
        out_specs=(P("dp", BLK, AA), P(BLK_AA)),
        check_vma=False,
    )
```

```python
import jax
import jax.numpy as jnp
from jax import lax
from jax.experimental import pallas as pl
from jax.experimental.pallas import tpu as pltpu
from jax.sharding import Mesh
from jax.sharding import PartitionSpec as P

DH = 128
BLK = ("blk_0", "blk_1")
AA = ("aa_0", "aa_1")
BLK_AA = ("blk_0", "blk_1", "aa_0", "aa_1")


def place(at_ref, n):
    at = at_ref[0]
    return lax.div(at, n), lax.rem(at, n)


def place(at_ref, n):
    at = at_ref[0]
    return lax.div(at, n), lax.rem(at, n)


def run_all(moves, sems):
    copies = [pltpu.make_async_copy(a, b, sems.at[i]) for i, (a, b) in enumerate(moves)]
    for copy in copies:
        copy.start()
    for copy in copies:
        copy.wait()


def lanes_of(ref, index, width):
    return ref.at[:, pl.ds(pl.multiple_of(index * width, width), width)]


def pack_far_kernel(n, at_ref, q_ref, k_ref, v_ref, kv_to, sems):
    side, x = place(at_ref, n)
    moves = [(lanes_of(q_ref, (1 - side) * n + x, 2 * DH), kv_to.at[n // 2])]
    for i in range(n // 2):
        head = (1 - side) * (n // 2) + i
        moves.append((lanes_of(k_ref, head, DH), kv_to.at[i, :, :DH]))
        moves.append((lanes_of(v_ref, head, DH), kv_to.at[i, :, DH:]))
    run_all(moves, sems)


def pack_kernel(n, at_ref, q_ref, k_ref, v_ref, g_ref, *refs):
    to, g_to, sems = refs[:n], refs[n], refs[n + 1]
    side, x = place(at_ref, n)
    wide = q_ref.shape[1] // (2 * n)
    moves = []
    chunk = g_ref.shape[-1]
    for z in range(g_ref.shape[1]):
        moves.append((g_ref.at[:, z], g_to.at[:, :, :, z * chunk : (z + 1) * chunk]))
    for hop in range(n):
        target = lax.rem(x + hop, n)
        head = side * (n // 2) + lax.div(target, 2)
        moves.append((lanes_of(q_ref, side * n + target, wide), to[hop].at[:, :wide]))
        moves.append((lanes_of(k_ref, head, DH), to[hop].at[:, wide : wide + DH]))
        moves.append((lanes_of(v_ref, head, DH), to[hop].at[:, wide + DH : wide + 2 * DH]))
        if hop:
            moves.append((lanes_of(q_ref, (1 - side) * n + target, wide), to[hop].at[:, wide + 2 * DH :]))
    run_all(moves, sems)


def kernel_call(body, outs, ins, name, scratch=(), limit=8 << 20, **more):
    vmem = pl.BlockSpec(memory_space=pltpu.VMEM)
    settings = dict(
        out_shape=outs,
        in_specs=[pl.BlockSpec(memory_space=pltpu.SMEM)] + [vmem] * (len(ins) - 1),
        out_specs=(vmem,) * len(outs),
        scratch_shapes=list(scratch),
        compiler_params=pltpu.CompilerParams(vmem_limit_bytes=limit),
        name=name,
    )
    settings.update(more)
    return pl.pallas_call(body, **settings)(*ins)


def packed_far(at, q, k, v, n):
    return kernel_call(
        lambda *refs: pack_far_kernel(n, *refs),
        (jax.ShapeDtypeStruct((n // 2 + 1, k.shape[0], 2 * DH), k.dtype),),
        (at, q, k, v),
        "pack_far",
        scratch=(pltpu.SemaphoreType.DMA((n + 1,)),),
        in_specs=[pl.BlockSpec(memory_space=pltpu.SMEM)] + [pl.BlockSpec(memory_space=pl.ANY)] * 3,
    )[0]


def packed(at, q, k, v, g, n):
    rows, wide = q.shape[0], q.shape[1] // (2 * n)
    yc, z, x, _, chunk = g.shape
    outs = (
        jax.ShapeDtypeStruct((rows, wide + 2 * DH), q.dtype),
        *(jax.ShapeDtypeStruct((rows, 2 * wide + 2 * DH), q.dtype),) * (n - 1),
        jax.ShapeDtypeStruct((yc, x, 1, z * chunk), g.dtype),
    )
    found = kernel_call(
        lambda *refs: pack_kernel(n, *refs),
        outs,
        (at, q, k, v, g),
        "pack",
        scratch=(pltpu.SemaphoreType.DMA((4 * n - 1 + z,)),),
        in_specs=[pl.BlockSpec(memory_space=pltpu.SMEM)] + [pl.BlockSpec(memory_space=pl.ANY)] * 4,
    )
    return found[:n], found[-1]


def stack_kernel(n, *refs):
    for hop in range(n):
        refs[n][hop] = refs[hop][:, -refs[n].shape[-1] :]


def stacked(pieces, wide):
    n, rows = len(pieces), pieces[0].shape[0]
    vmem = pl.BlockSpec(memory_space=pltpu.VMEM)
    return kernel_call(
        lambda *refs: stack_kernel(n, *refs),
        (jax.ShapeDtypeStruct((n, rows, wide), pieces[0].dtype),),
        tuple(pieces),
        "stack",
        in_specs=[vmem] * n,
    )[0]


def cut_kernel(n, at_ref, kv_ref, *to):
    _, x = place(at_ref, n)
    for hop in range(n):
        to[hop][...] = kv_ref[lax.div(lax.rem(x + hop, n), 2)]


def cut(at, kv, n):
    outs = (jax.ShapeDtypeStruct(kv.shape[1:], kv.dtype),) * n
    return kernel_call(lambda *refs: cut_kernel(n, *refs), outs, (at, kv), "cut")


def gather_kernel(n, at_ref, *refs):
    near, far, (kv_ref, last_ref) = refs[:n], refs[n : 2 * n], refs[2 * n :]
    side, x = place(at_ref, n)
    rows, width = far[0].shape

    def put(half, chunk, value):
        kv_ref[pl.ds(pl.multiple_of((half * n + chunk) * rows, rows), rows)] = value

    for hop in range(n):
        chunk = lax.rem(x + n - hop, n)
        wide = near[0].shape[1] - width
        put(side, chunk, near[hop][:, wide : wide + width])
        put(1 - side, chunk, far[hop][...])
    last_ref[...] = kv_ref[kv_ref.shape[0] - last_ref.shape[0] :]


def gathered(at, near, far, reach):
    rows, width = far[0].shape
    n = len(near)
    outs = (
        jax.ShapeDtypeStruct((2 * n * rows, width), jnp.bfloat16),
        jax.ShapeDtypeStruct((reach, width), jnp.bfloat16),
    )
    return kernel_call(lambda *refs: gather_kernel(n, *refs), outs, (at, *near, *far), "gather")


def attend_kernel(n, is_near, count, at_ref, kv_ref, prior_ref, *refs):
    pieces, out_ref, q_s, older_s, out_s, sem = refs[:count], *refs[-5:]
    side, x = place(at_ref, n)
    half = side if is_near else 1 - side
    rows, wide = q_s.shape[0] // n, q_s.shape[1]
    reach = prior_ref.shape[0]
    for hop in range(n):
        chunk = lax.rem(x + n - hop, n)
        value = pieces[hop][:, :wide] if is_near else pieces[0][hop - 1] if hop else pieces[1][n // 2]
        q_s[pl.ds(pl.multiple_of(chunk * rows, rows), rows)] = value
    start = pl.multiple_of(half * n * rows, reach)

    @pl.when(half == 0)
    def _():
        older_s[...] = prior_ref[...]

    @pl.when(half != 0)
    def _():
        older_s[...] = kv_ref[n * rows - reach : n * rows]

    row = lax.broadcasted_iota(jnp.int32, (reach, reach), 0)
    col = lax.broadcasted_iota(jnp.int32, (reach, reach), 1)
    newer = col <= row
    across = (((1,), (1,)), ((), ()))
    for block in range(n * rows // reach):
        here = pl.ds(block * reach, reach)
        now = pl.ds(pl.multiple_of(start + block * reach, reach), reach)
        if block:
            older_ref, older = kv_ref, pl.ds(pl.multiple_of(start + (block - 1) * reach, reach), reach)
        else:
            older_ref, older = older_s, slice(None)
        for head in range(wide // DH):
            lanes = pl.ds(head * DH, DH)
            q = q_s[here, lanes]
            old = lax.dot_general(q, older_ref[older, :DH], across, preferred_element_type=jnp.float32)
            new = lax.dot_general(q, kv_ref[now, :DH], across, preferred_element_type=jnp.float32)
            scores = jnp.where(newer, new, old) * DH**-0.5
            expo = jnp.exp(scores - jnp.max(scores, axis=-1, keepdims=True))
            weights = (expo / jnp.sum(expo, axis=-1, keepdims=True)).astype(jnp.bfloat16)
            none = jnp.zeros_like(weights)
            out = jnp.dot(
                jnp.where(newer, weights, none), kv_ref[now, DH:], preferred_element_type=jnp.float32
            ) + jnp.dot(
                jnp.where(newer, none, weights), older_ref[older, DH:], preferred_element_type=jnp.float32
            )
            out_s[here, lanes] = out.astype(jnp.bfloat16)
    copy = pltpu.make_async_copy(out_s, out_ref.at[pl.ds(start, n * rows)], sem)
    copy.start()
    copy.wait()


def attended_half(at, kv, prior, pieces, n, wide, onto=None):
    reach, total = prior.shape[0], kv.shape[0]
    vmem, somewhere = pl.BlockSpec(memory_space=pltpu.VMEM), pl.BlockSpec(memory_space=pl.ANY)
    is_near = onto is None
    ins = (at, kv, prior, *pieces) + (() if is_near else (onto,))
    return kernel_call(
        lambda *refs: attend_kernel(n, is_near, len(pieces), *refs),
        (jax.ShapeDtypeStruct((total, wide), jnp.bfloat16),),
        ins,
        "attend",
        scratch=(
            pltpu.VMEM((total // 2, wide), jnp.bfloat16),
            pltpu.VMEM(prior.shape, jnp.bfloat16),
            pltpu.VMEM((total // 2, wide), jnp.bfloat16),
            pltpu.SemaphoreType.DMA,
        ),
        limit=16 << 20,
        in_specs=[pl.BlockSpec(memory_space=pltpu.SMEM)]
        + [vmem] * (2 + len(pieces))
        + ([] if is_near else [somewhere]),
        out_specs=(somewhere,),
        input_output_aliases={} if is_near else {3 + len(pieces): 0},
        cost_estimate=pl.CostEstimate(
            flops=4 * total * wide * reach, bytes_accessed=2 * total * wide * 2, transcendentals=total * reach
        ),
    )[0]


def step(queries, keys, values, grad_parts):
    dp, y, c, z, n = (lax.axis_size(a) for a in ("dp", *BLK_AA))
    at = lax.axis_index(AA).astype(jnp.int32).reshape(1)
    wide = queries.shape[2] // (z * n)
    reach = queries.shape[1] * 2
    chunks = grad_parts.reshape(y * c, z, n, 1, -1)
    kv_far = packed_far(at, queries[0], keys[0], values[0], n)
    sent, parts = packed(at, queries[0], keys[0], values[0], chunks, n)

    def along_x(value, hop):
        return lax.ppermute(value, "aa_1", [(x, (x + hop) % n) for x in range(n)])

    def across_z(value):
        return lax.ppermute(value, "aa_0", [(s, 1 - s) for s in range(z)])

    kv_far = across_z(kv_far)
    near = [sent[0]] + [along_x(sent[hop], hop) for hop in range(1, n)]
    parts = parts.reshape(y * c * n, 1, -1)
    parts = lax.all_to_all(parts, ("blk_0", "blk_1", "aa_1"), 0, 0, tiled=True)
    q_far = stacked(near[1:], wide)
    q_far = across_z(q_far)
    far = cut(at, kv_far, n)
    far = [far[0]] + [along_x(far[hop], hop) for hop in range(1, n)]
    kv, last = gathered(at, near, far, reach)
    prior = lax.ppermute(last, BLK, [(i, i + 1) for i in range(y * c - 1)])
    rows = attended_half(at, kv, prior, near, n, wide)

    share = jnp.sum(parts, axis=0).reshape(z, 1, -1)
    share = jnp.broadcast_to(share[None], (dp, *share.shape)).reshape(dp * z, 1, -1)
    share = lax.all_to_all(share, ("dp", "aa_0"), 0, 0, tiled=True)
    grad_mean = jnp.sum(share, axis=(0, 1)) / (dp * y * c * z * n)

    rows = attended_half(at, kv, prior, (q_far, kv_far), n, wide, rows)
    return rows[None], grad_mean


def solution(mesh):
    torus = Mesh(
        mesh.devices.reshape(mesh.shape["dp"], 8, 2, 2, 4), ("dp", "blk_0", "blk_1", "aa_0", "aa_1")
    )
    placed = P("dp", BLK_AA, None)
    return jax.shard_map(
        step,
        mesh=torus,
        in_specs=(placed,) * 4,
        out_specs=(P("dp", BLK, AA), P(BLK_AA)),
        check_vma=False,
    )
```

```python
import jax
import jax.numpy as jnp
from jax import lax
from jax.experimental import pallas as pl
from jax.experimental.pallas import tpu as pltpu
from jax.sharding import Mesh
from jax.sharding import PartitionSpec as P

DH = 128
BLK = ("blk_0", "blk_1")
AA = ("aa_0", "aa_1")
BLK_AA = ("blk_0", "blk_1", "aa_0", "aa_1")


def place(at_ref, n):
    at = at_ref[0]
    return lax.div(at, n), lax.rem(at, n)


def place(at_ref, n):
    at = at_ref[0]
    return lax.div(at, n), lax.rem(at, n)


def run_all(moves, sems):
    copies = [pltpu.make_async_copy(a, b, sems.at[i]) for i, (a, b) in enumerate(moves)]
    for copy in copies:
        copy.start()
    for copy in copies:
        copy.wait()


def lanes_of(ref, index, width):
    return ref.at[:, pl.ds(pl.multiple_of(index * width, width), width)]


def pack_far_kernel(n, at_ref, q_ref, k_ref, v_ref, kv_to, sems):
    side, x = place(at_ref, n)
    moves = [(lanes_of(q_ref, (1 - side) * n + x, 2 * DH), kv_to.at[n // 2])]
    for i in range(n // 2):
        head = (1 - side) * (n // 2) + i
        moves.append((lanes_of(k_ref, head, DH), kv_to.at[i, :, :DH]))
        moves.append((lanes_of(v_ref, head, DH), kv_to.at[i, :, DH:]))
    run_all(moves, sems)


def pack_kernel(n, at_ref, q_ref, k_ref, v_ref, to, sems):
    side, _ = place(at_ref, n)
    wide = q_ref.shape[1] // (2 * n)
    moves = []
    for target in range(n):
        head = side * (n // 2) + target // 2
        moves.append((lanes_of(q_ref, side * n + target, wide), to.at[target, :, :wide]))
        moves.append((lanes_of(k_ref, head, DH), to.at[target, :, wide : wide + DH]))
        moves.append((lanes_of(v_ref, head, DH), to.at[target, :, wide + DH : wide + 2 * DH]))
        moves.append((lanes_of(q_ref, (1 - side) * n + target, wide), to.at[target, :, wide + 2 * DH :]))
    run_all(moves, sems)


def pack_parts_kernel(_, g_ref, g_to, sems):
    chunk = g_ref.shape[-1]
    moves = [(g_ref.at[:, z], g_to.at[:, :, :, z * chunk : (z + 1) * chunk]) for z in range(g_ref.shape[1])]
    run_all(moves, sems)


def kernel_call(body, outs, ins, name, scratch=(), limit=8 << 20, **more):
    vmem = pl.BlockSpec(memory_space=pltpu.VMEM)
    settings = dict(
        out_shape=outs,
        in_specs=[pl.BlockSpec(memory_space=pltpu.SMEM)] + [vmem] * (len(ins) - 1),
        out_specs=(vmem,) * len(outs),
        scratch_shapes=list(scratch),
        compiler_params=pltpu.CompilerParams(vmem_limit_bytes=limit),
        name=name,
    )
    settings.update(more)
    return pl.pallas_call(body, **settings)(*ins)


def packed_far(at, q, k, v, n):
    return kernel_call(
        lambda *refs: pack_far_kernel(n, *refs),
        (jax.ShapeDtypeStruct((n // 2 + 1, k.shape[0], 2 * DH), k.dtype),),
        (at, q, k, v),
        "pack_far",
        scratch=(pltpu.SemaphoreType.DMA((n + 1,)),),
        in_specs=[pl.BlockSpec(memory_space=pltpu.SMEM)] + [pl.BlockSpec(memory_space=pl.ANY)] * 3,
    )[0]


def packed(at, q, k, v, n):
    rows, wide = q.shape[0], q.shape[1] // (2 * n)
    return kernel_call(
        lambda *refs: pack_kernel(n, *refs),
        (jax.ShapeDtypeStruct((n, rows, 2 * wide + 2 * DH), q.dtype),),
        (at, q, k, v),
        "pack",
        scratch=(pltpu.SemaphoreType.DMA((4 * n,)),),
        in_specs=[pl.BlockSpec(memory_space=pltpu.SMEM)] + [pl.BlockSpec(memory_space=pl.ANY)] * 3,
    )[0]


def packed_parts(at, g):
    yc, z, x, _, chunk = g.shape
    return kernel_call(
        pack_parts_kernel,
        (jax.ShapeDtypeStruct((yc, x, 1, z * chunk), g.dtype),),
        (at, g),
        "pack_parts",
        scratch=(pltpu.SemaphoreType.DMA((z,)),),
        in_specs=[pl.BlockSpec(memory_space=pltpu.SMEM), pl.BlockSpec(memory_space=pl.ANY)],
    )[0]


def stack_kernel(n, at_ref, near_ref, to):
    _, x = place(at_ref, n)
    for hop in range(1, n):
        to[hop - 1] = near_ref[lax.rem(x + n - hop, n), :, -to.shape[-1] :]


def stacked(at, near, wide):
    n, rows = near.shape[:2]
    outs = (jax.ShapeDtypeStruct((n - 1, rows, wide), near.dtype),)
    return kernel_call(lambda *refs: stack_kernel(n, *refs), outs, (at, near), "stack")[0]


def cut_kernel(n, at_ref, kv_ref, *to):
    _, x = place(at_ref, n)
    for hop in range(n):
        to[hop][...] = kv_ref[lax.div(lax.rem(x + hop, n), 2)]


def cut(at, kv, n):
    outs = (jax.ShapeDtypeStruct(kv.shape[1:], kv.dtype),) * n
    return kernel_call(lambda *refs: cut_kernel(n, *refs), outs, (at, kv), "cut")


def gather_kernel(n, at_ref, *refs):
    near_ref, far, (kv_ref, last_ref) = refs[0], refs[1 : n + 1], refs[n + 1 :]
    side, x = place(at_ref, n)
    rows, width = far[0].shape

    def put(half, chunk, value):
        kv_ref[pl.ds(pl.multiple_of((half * n + chunk) * rows, rows), rows)] = value

    wide = (near_ref.shape[-1] - width) // 2
    for hop in range(n):
        put(side, hop, near_ref[hop, :, wide : wide + width])
        put(1 - side, lax.rem(x + n - hop, n), far[hop][...])
    last_ref[...] = kv_ref[kv_ref.shape[0] - last_ref.shape[0] :]


def gathered(at, near, far, reach):
    rows, width = far[0].shape
    n = len(far)
    outs = (
        jax.ShapeDtypeStruct((2 * n * rows, width), jnp.bfloat16),
        jax.ShapeDtypeStruct((reach, width), jnp.bfloat16),
    )
    return kernel_call(lambda *refs: gather_kernel(n, *refs), outs, (at, near, *far), "gather")


def attend_kernel(n, is_near, count, at_ref, kv_ref, prior_ref, *refs):
    pieces, out_ref, q_s, older_s, out_s, sem = refs[:count], *refs[-5:]
    side, x = place(at_ref, n)
    half = side if is_near else 1 - side
    rows, wide = q_s.shape[0] // n, q_s.shape[1]
    reach = prior_ref.shape[0]
    for hop in range(n):
        chunk = hop if is_near else lax.rem(x + n - hop, n)
        value = pieces[0][hop, :, :wide] if is_near else pieces[0][hop - 1] if hop else pieces[1][n // 2]
        q_s[pl.ds(pl.multiple_of(chunk * rows, rows), rows)] = value
    start = pl.multiple_of(half * n * rows, reach)

    @pl.when(half == 0)
    def _():
        older_s[...] = prior_ref[...]

    @pl.when(half != 0)
    def _():
        older_s[...] = kv_ref[n * rows - reach : n * rows]

    row = lax.broadcasted_iota(jnp.int32, (reach, reach), 0)
    col = lax.broadcasted_iota(jnp.int32, (reach, reach), 1)
    newer = col <= row
    across = (((1,), (1,)), ((), ()))
    for block in range(n * rows // reach):
        here = pl.ds(block * reach, reach)
        now = pl.ds(pl.multiple_of(start + block * reach, reach), reach)
        if block:
            older_ref, older = kv_ref, pl.ds(pl.multiple_of(start + (block - 1) * reach, reach), reach)
        else:
            older_ref, older = older_s, slice(None)
        for head in range(wide // DH):
            lanes = pl.ds(head * DH, DH)
            q = q_s[here, lanes]
            old = lax.dot_general(q, older_ref[older, :DH], across, preferred_element_type=jnp.float32)
            new = lax.dot_general(q, kv_ref[now, :DH], across, preferred_element_type=jnp.float32)
            scores = jnp.where(newer, new, old) * DH**-0.5
            expo = jnp.exp(scores - jnp.max(scores, axis=-1, keepdims=True))
            weights = (expo / jnp.sum(expo, axis=-1, keepdims=True)).astype(jnp.bfloat16)
            none = jnp.zeros_like(weights)
            out = jnp.dot(
                jnp.where(newer, weights, none), kv_ref[now, DH:], preferred_element_type=jnp.float32
            ) + jnp.dot(
                jnp.where(newer, none, weights), older_ref[older, DH:], preferred_element_type=jnp.float32
            )
            out_s[here, lanes] = out.astype(jnp.bfloat16)
    copy = pltpu.make_async_copy(out_s, out_ref.at[pl.ds(start, n * rows)], sem)
    copy.start()
    copy.wait()


def attended_half(at, kv, prior, pieces, n, wide, onto=None):
    reach, total = prior.shape[0], kv.shape[0]
    vmem, somewhere = pl.BlockSpec(memory_space=pltpu.VMEM), pl.BlockSpec(memory_space=pl.ANY)
    is_near = onto is None
    ins = (at, kv, prior, *pieces) + (() if is_near else (onto,))
    return kernel_call(
        lambda *refs: attend_kernel(n, is_near, len(pieces), *refs),
        (jax.ShapeDtypeStruct((total, wide), jnp.bfloat16),),
        ins,
        "attend",
        scratch=(
            pltpu.VMEM((total // 2, wide), jnp.bfloat16),
            pltpu.VMEM(prior.shape, jnp.bfloat16),
            pltpu.VMEM((total // 2, wide), jnp.bfloat16),
            pltpu.SemaphoreType.DMA,
        ),
        limit=16 << 20,
        in_specs=[pl.BlockSpec(memory_space=pltpu.SMEM)]
        + [vmem] * (2 + len(pieces))
        + ([] if is_near else [somewhere]),
        out_specs=(somewhere,),
        input_output_aliases={} if is_near else {3 + len(pieces): 0},
        cost_estimate=pl.CostEstimate(
            flops=4 * total * wide * reach, bytes_accessed=2 * total * wide * 2, transcendentals=total * reach
        ),
    )[0]


def step(queries, keys, values, grad_parts):
    dp, y, c, z, n = (lax.axis_size(a) for a in ("dp", *BLK_AA))
    at = lax.axis_index(AA).astype(jnp.int32).reshape(1)
    wide = queries.shape[2] // (z * n)
    reach = queries.shape[1] * 2
    chunks = grad_parts.reshape(y * c, z, n, 1, -1)
    local = queries[0], keys[0], values[0]
    kv_far = packed_far(at, *local, n)
    sent = packed(at, *local, n)
    parts = packed_parts(at, chunks)

    def along_x(value, hop):
        return lax.ppermute(value, "aa_1", [(x, (x + hop) % n) for x in range(n)])

    def across_z(value):
        return lax.ppermute(value, "aa_0", [(s, 1 - s) for s in range(z)])

    near = lax.all_to_all(sent, "aa_1", 0, 0, tiled=True)
    kv_far = across_z(kv_far)
    parts = parts.reshape(y * c * n, 1, -1)
    parts = lax.all_to_all(parts, ("blk_0", "blk_1", "aa_1"), 0, 0, tiled=True)
    q_far = stacked(at, near, wide)
    q_far = across_z(q_far)
    far = cut(at, kv_far, n)
    far = [far[0]] + [along_x(far[hop], hop) for hop in range(1, n)]
    kv, last = gathered(at, near, far, reach)
    prior = lax.ppermute(last, BLK, [(i, i + 1) for i in range(y * c - 1)])
    rows = attended_half(at, kv, prior, (near,), n, wide)

    share = jnp.sum(parts, axis=0).reshape(z, 1, -1)
    share = jnp.broadcast_to(share[None], (dp, *share.shape)).reshape(dp * z, 1, -1)
    share = lax.all_to_all(share, ("dp", "aa_0"), 0, 0, tiled=True)
    grad_mean = jnp.sum(share, axis=(0, 1)) / (dp * y * c * z * n)

    rows = attended_half(at, kv, prior, (q_far, kv_far), n, wide, rows)
    return rows[None], grad_mean


def solution(mesh):
    torus = Mesh(
        mesh.devices.reshape(mesh.shape["dp"], 8, 2, 2, 4), ("dp", "blk_0", "blk_1", "aa_0", "aa_1")
    )
    placed = P("dp", BLK_AA, None)
    return jax.shard_map(
        step,
        mesh=torus,
        in_specs=(placed,) * 4,
        out_specs=(P("dp", BLK, AA), P(BLK_AA)),
        check_vma=False,
    )
```

```python
import jax
import jax.numpy as jnp
from jax import lax
from jax.experimental import pallas as pl
from jax.experimental.pallas import tpu as pltpu
from jax.sharding import Mesh
from jax.sharding import PartitionSpec as P

DH = 128
BLK = ("blk_0", "blk_1")
AA = ("aa_0", "aa_1")
BLK_AA = ("blk_0", "blk_1", "aa_0", "aa_1")


def place(at_ref, n):
    at = at_ref[0]
    return lax.div(at, n), lax.rem(at, n)


def place(at_ref, n):
    at = at_ref[0]
    return lax.div(at, n), lax.rem(at, n)


def run_all(moves, sems):
    copies = [pltpu.make_async_copy(a, b, sems.at[i]) for i, (a, b) in enumerate(moves)]
    for copy in copies:
        copy.start()
    for copy in copies:
        copy.wait()


def lanes_of(ref, index, width):
    return ref.at[:, pl.ds(pl.multiple_of(index * width, width), width)]


def pack_far_kernel(n, at_ref, q_ref, k_ref, v_ref, kv_to, sems):
    side, x = place(at_ref, n)
    moves = [(lanes_of(q_ref, (1 - side) * n + x, 2 * DH), kv_to.at[n // 2])]
    for i in range(n // 2):
        head = (1 - side) * (n // 2) + i
        moves.append((lanes_of(k_ref, head, DH), kv_to.at[i, :, :DH]))
        moves.append((lanes_of(v_ref, head, DH), kv_to.at[i, :, DH:]))
    run_all(moves, sems)


def pack_kernel(n, at_ref, q_ref, k_ref, v_ref, far_to, to, sems):
    side, _ = place(at_ref, n)
    wide = q_ref.shape[1] // (2 * n)
    moves = []
    for target in range(n):
        head = side * (n // 2) + target // 2
        moves.append((lanes_of(q_ref, side * n + target, wide), to.at[target, :, :wide]))
        moves.append((lanes_of(k_ref, head, DH), to.at[target, :, wide : wide + DH]))
        moves.append((lanes_of(v_ref, head, DH), to.at[target, :, wide + DH : wide + 2 * DH]))
        moves.append((lanes_of(q_ref, (1 - side) * n + target, wide), far_to.at[target]))
    run_all(moves, sems)


def pack_parts_kernel(_, g_ref, g_to, sems):
    chunk = g_ref.shape[-1]
    moves = [(g_ref.at[:, z], g_to.at[:, :, :, z * chunk : (z + 1) * chunk]) for z in range(g_ref.shape[1])]
    run_all(moves, sems)


def kernel_call(body, outs, ins, name, scratch=(), limit=8 << 20, **more):
    vmem = pl.BlockSpec(memory_space=pltpu.VMEM)
    settings = dict(
        out_shape=outs,
        in_specs=[pl.BlockSpec(memory_space=pltpu.SMEM)] + [vmem] * (len(ins) - 1),
        out_specs=(vmem,) * len(outs),
        scratch_shapes=list(scratch),
        compiler_params=pltpu.CompilerParams(vmem_limit_bytes=limit),
        name=name,
    )
    settings.update(more)
    return pl.pallas_call(body, **settings)(*ins)


def packed_far(at, q, k, v, n):
    return kernel_call(
        lambda *refs: pack_far_kernel(n, *refs),
        (jax.ShapeDtypeStruct((n // 2 + 1, k.shape[0], 2 * DH), k.dtype),),
        (at, q, k, v),
        "pack_far",
        limit=60 << 20,
        scratch=(pltpu.SemaphoreType.DMA((n + 1,)),),
        in_specs=[pl.BlockSpec(memory_space=pltpu.SMEM)] + [pl.BlockSpec(memory_space=pl.ANY)] * 3,
    )[0]


def packed(at, q, k, v, n):
    rows, wide = q.shape[0], q.shape[1] // (2 * n)
    return kernel_call(
        lambda *refs: pack_kernel(n, *refs),
        (
            jax.ShapeDtypeStruct((n, rows, wide), q.dtype),
            jax.ShapeDtypeStruct((n, rows, wide + 2 * DH), q.dtype),
        ),
        (at, q, k, v),
        "pack",
        scratch=(pltpu.SemaphoreType.DMA((4 * n,)),),
        in_specs=[pl.BlockSpec(memory_space=pltpu.SMEM)] + [pl.BlockSpec(memory_space=pl.ANY)] * 3,
    )


def packed_parts(at, g):
    yc, z, x, _, chunk = g.shape
    return kernel_call(
        pack_parts_kernel,
        (jax.ShapeDtypeStruct((yc, x, 1, z * chunk), g.dtype),),
        (at, g),
        "pack_parts",
        limit=60 << 20,
        scratch=(pltpu.SemaphoreType.DMA((z,)),),
        in_specs=[pl.BlockSpec(memory_space=pltpu.SMEM), pl.BlockSpec(memory_space=pl.ANY)],
    )[0]


def stack_kernel(n, at_ref, near_ref, to):
    _, x = place(at_ref, n)
    for hop in range(1, n):
        to[hop - 1] = near_ref[lax.rem(x + n - hop, n), :, -to.shape[-1] :]


def stacked(at, near, wide):
    n, rows = near.shape[:2]
    outs = (jax.ShapeDtypeStruct((n - 1, rows, wide), near.dtype),)
    return kernel_call(lambda *refs: stack_kernel(n, *refs), outs, (at, near), "stack")[0]


def cut_kernel(n, at_ref, near_ref, kv_ref, *to):
    _, x = place(at_ref, n)
    for hop in range(n):
        target = lax.rem(x + hop, n)
        to[hop][:, : near_ref.shape[-1]] = near_ref[target]
        to[hop][:, near_ref.shape[-1] :] = kv_ref[lax.div(target, 2)]


def cut(at, near, kv):
    n, rows, wide = near.shape
    outs = (jax.ShapeDtypeStruct((rows, wide + kv.shape[-1]), kv.dtype),) * n
    return kernel_call(lambda *refs: cut_kernel(n, *refs), outs, (at, near, kv), "cut")


def gather_kernel(n, at_ref, *refs):
    both, (kv_ref, last_ref) = refs[:n], refs[n:]
    side, x = place(at_ref, n)
    rows, width = both[0].shape[0], kv_ref.shape[1]

    def put(half, chunk, value):
        kv_ref[pl.ds(pl.multiple_of((half * n + chunk) * rows, rows), rows)] = value

    for hop in range(n):
        chunk = lax.rem(x + n - hop, n)
        put(side, chunk, both[hop][:, -2 * width : -width])
        put(1 - side, chunk, both[hop][:, -width:])
    last_ref[...] = kv_ref[kv_ref.shape[0] - last_ref.shape[0] :]


def gathered(at, both, reach):
    n, rows = len(both), both[0].shape[0]
    outs = (
        jax.ShapeDtypeStruct((2 * n * rows, 2 * DH), jnp.bfloat16),
        jax.ShapeDtypeStruct((reach, 2 * DH), jnp.bfloat16),
    )
    return kernel_call(lambda *refs: gather_kernel(n, *refs), outs, (at, *both), "gather")


def attend_kernel(n, is_near, count, at_ref, kv_ref, prior_ref, *refs):
    pieces, out_ref, q_s, older_s, out_s, sem = refs[:count], *refs[-5:]
    side, x = place(at_ref, n)
    half = side if is_near else 1 - side
    rows, wide = q_s.shape[0] // n, q_s.shape[1]
    reach = prior_ref.shape[0]
    for hop in range(n):
        chunk = lax.rem(x + n - hop, n)
        value = pieces[hop][:, :wide] if is_near else pieces[0][hop - 1] if hop else pieces[1][n // 2]
        q_s[pl.ds(pl.multiple_of(chunk * rows, rows), rows)] = value
    start = pl.multiple_of(half * n * rows, reach)

    @pl.when(half == 0)
    def _():
        older_s[...] = prior_ref[...]

    @pl.when(half != 0)
    def _():
        older_s[...] = kv_ref[n * rows - reach : n * rows]

    row = lax.broadcasted_iota(jnp.int32, (reach, reach), 0)
    col = lax.broadcasted_iota(jnp.int32, (reach, reach), 1)
    newer = col <= row
    across = (((1,), (1,)), ((), ()))
    for block in range(n * rows // reach):
        here = pl.ds(block * reach, reach)
        now = pl.ds(pl.multiple_of(start + block * reach, reach), reach)
        if block:
            older_ref, older = kv_ref, pl.ds(pl.multiple_of(start + (block - 1) * reach, reach), reach)
        else:
            older_ref, older = older_s, slice(None)
        for head in range(wide // DH):
            lanes = pl.ds(head * DH, DH)
            q = q_s[here, lanes]
            old = lax.dot_general(q, older_ref[older, :DH], across, preferred_element_type=jnp.float32)
            new = lax.dot_general(q, kv_ref[now, :DH], across, preferred_element_type=jnp.float32)
            scores = jnp.where(newer, new, old) * DH**-0.5
            expo = jnp.exp(scores - jnp.max(scores, axis=-1, keepdims=True))
            weights = (expo / jnp.sum(expo, axis=-1, keepdims=True)).astype(jnp.bfloat16)
            none = jnp.zeros_like(weights)
            out = jnp.dot(
                jnp.where(newer, weights, none), kv_ref[now, DH:], preferred_element_type=jnp.float32
            ) + jnp.dot(
                jnp.where(newer, none, weights), older_ref[older, DH:], preferred_element_type=jnp.float32
            )
            out_s[here, lanes] = out.astype(jnp.bfloat16)
    copy = pltpu.make_async_copy(out_s, out_ref.at[pl.ds(start, n * rows)], sem)
    copy.start()
    copy.wait()


def attended_half(at, kv, prior, pieces, n, wide, onto=None):
    reach, total = prior.shape[0], kv.shape[0]
    vmem, somewhere = pl.BlockSpec(memory_space=pltpu.VMEM), pl.BlockSpec(memory_space=pl.ANY)
    is_near = onto is None
    ins = (at, kv, prior, *pieces) + (() if is_near else (onto,))
    return kernel_call(
        lambda *refs: attend_kernel(n, is_near, len(pieces), *refs),
        (jax.ShapeDtypeStruct((total, wide), jnp.bfloat16),),
        ins,
        "attend",
        scratch=(
            pltpu.VMEM((total // 2, wide), jnp.bfloat16),
            pltpu.VMEM(prior.shape, jnp.bfloat16),
            pltpu.VMEM((total // 2, wide), jnp.bfloat16),
            pltpu.SemaphoreType.DMA,
        ),
        limit=16 << 20,
        in_specs=[pl.BlockSpec(memory_space=pltpu.SMEM)]
        + [vmem] * (2 + len(pieces))
        + ([] if is_near else [somewhere]),
        out_specs=(somewhere,),
        input_output_aliases={} if is_near else {3 + len(pieces): 0},
        cost_estimate=pl.CostEstimate(
            flops=4 * total * wide * reach, bytes_accessed=2 * total * wide * 2, transcendentals=total * reach
        ),
    )[0]


def step(queries, keys, values, grad_parts):
    dp, y, c, z, n = (lax.axis_size(a) for a in ("dp", *BLK_AA))
    at = lax.axis_index(AA).astype(jnp.int32).reshape(1)
    wide = queries.shape[2] // (z * n)
    reach = queries.shape[1] * 2
    chunks = grad_parts.reshape(y * c, z, n, 1, -1)
    local = queries[0], keys[0], values[0]
    kv_far = packed_far(at, *local, n)
    sent, near = packed(at, *local, n)
    parts = packed_parts(at, chunks)

    def along_x(value, hop):
        return lax.ppermute(value, "aa_1", [(x, (x + hop) % n) for x in range(n)])

    def across_z(value):
        return lax.ppermute(value, "aa_0", [(s, 1 - s) for s in range(z)])

    q_far = lax.all_to_all(sent, "aa_1", 0, 0, tiled=True)
    kv_far = across_z(kv_far)
    parts = parts.reshape(y * c * n, 1, -1)
    parts = lax.all_to_all(parts, ("blk_0", "blk_1", "aa_1"), 0, 0, tiled=True)
    q_far = stacked(at, q_far, wide)
    q_far = across_z(q_far)
    both = cut(at, near, kv_far)
    both = [both[0]] + [along_x(both[hop], hop) for hop in range(1, n)]
    kv, last = gathered(at, both, reach)
    prior = lax.ppermute(last, BLK, [(i, i + 1) for i in range(y * c - 1)])
    rows = attended_half(at, kv, prior, both, n, wide)

    share = jnp.sum(parts, axis=0).reshape(z, 1, -1)
    share = jnp.broadcast_to(share[None], (dp, *share.shape)).reshape(dp * z, 1, -1)
    share = lax.all_to_all(share, ("dp", "aa_0"), 0, 0, tiled=True)
    grad_mean = jnp.sum(share, axis=(0, 1)) / (dp * y * c * z * n)

    rows = attended_half(at, kv, prior, (q_far, kv_far), n, wide, rows)
    return rows[None], grad_mean


def solution(mesh):
    torus = Mesh(
        mesh.devices.reshape(mesh.shape["dp"], 8, 2, 2, 4), ("dp", "blk_0", "blk_1", "aa_0", "aa_1")
    )
    placed = P("dp", BLK_AA, None)
    return jax.shard_map(
        step,
        mesh=torus,
        in_specs=(placed,) * 4,
        out_specs=(P("dp", BLK, AA), P(BLK_AA)),
        check_vma=False,
    )
```

```python
import jax
import jax.numpy as jnp
from jax import lax
from jax.experimental import pallas as pl
from jax.experimental.pallas import tpu as pltpu
from jax.sharding import Mesh
from jax.sharding import PartitionSpec as P

DH = 128
BLK = ("blk_0", "blk_1")
AA = ("aa_0", "aa_1")
BLK_AA = ("blk_0", "blk_1", "aa_0", "aa_1")


def place(at_ref, n):
    at = at_ref[0]
    return lax.div(at, n), lax.rem(at, n)


def place(at_ref, n):
    at = at_ref[0]
    return lax.div(at, n), lax.rem(at, n)


def run_all(moves, sems):
    copies = [pltpu.make_async_copy(a, b, sems.at[i]) for i, (a, b) in enumerate(moves)]
    for copy in copies:
        copy.start()
    for copy in copies:
        copy.wait()


def lanes_of(ref, index, width):
    return ref.at[:, pl.ds(pl.multiple_of(index * width, width), width)]


def pack_far_kernel(n, at_ref, q_ref, k_ref, v_ref, kv_to, sems):
    side, x = place(at_ref, n)
    moves = [(lanes_of(q_ref, (1 - side) * n + x, 2 * DH), kv_to.at[n // 2])]
    for i in range(n // 2):
        head = (1 - side) * (n // 2) + i
        moves.append((lanes_of(k_ref, head, DH), kv_to.at[i, :, :DH]))
        moves.append((lanes_of(v_ref, head, DH), kv_to.at[i, :, DH:]))
    run_all(moves, sems)


def pack_kernel(n, at_ref, q_ref, k_ref, v_ref, g_ref, *refs):
    to, g_to, sems = refs[:n], refs[n], refs[n + 1]
    side, x = place(at_ref, n)
    wide = q_ref.shape[1] // (2 * n)
    moves = []
    chunk = g_ref.shape[-1]
    for z in range(g_ref.shape[1]):
        moves.append((g_ref.at[:, z], g_to.at[:, :, :, z * chunk : (z + 1) * chunk]))
    for hop in range(n):
        target = lax.rem(x + hop, n)
        head = side * (n // 2) + lax.div(target, 2)
        moves.append((lanes_of(q_ref, side * n + target, wide), to[hop].at[:, :wide]))
        moves.append((lanes_of(k_ref, head, DH), to[hop].at[:, wide : wide + DH]))
        moves.append((lanes_of(v_ref, head, DH), to[hop].at[:, wide + DH : wide + 2 * DH]))
        if hop:
            moves.append((lanes_of(q_ref, (1 - side) * n + target, wide), to[hop].at[:, wide + 2 * DH :]))
    run_all(moves, sems)


def kernel_call(body, outs, ins, name, scratch=(), limit=8 << 20, **more):
    vmem = pl.BlockSpec(memory_space=pltpu.VMEM)
    settings = dict(
        out_shape=outs,
        in_specs=[pl.BlockSpec(memory_space=pltpu.SMEM)] + [vmem] * (len(ins) - 1),
        out_specs=(vmem,) * len(outs),
        scratch_shapes=list(scratch),
        compiler_params=pltpu.CompilerParams(vmem_limit_bytes=limit),
        name=name,
    )
    settings.update(more)
    return pl.pallas_call(body, **settings)(*ins)


def packed_far(at, q, k, v, n):
    return kernel_call(
        lambda *refs: pack_far_kernel(n, *refs),
        (jax.ShapeDtypeStruct((n // 2 + 1, k.shape[0], 2 * DH), k.dtype),),
        (at, q, k, v),
        "pack_far",
        limit=60 << 20,
        scratch=(pltpu.SemaphoreType.DMA((n + 1,)),),
        in_specs=[pl.BlockSpec(memory_space=pltpu.SMEM)] + [pl.BlockSpec(memory_space=pl.ANY)] * 3,
    )[0]


def packed(at, q, k, v, g, n):
    rows, wide = q.shape[0], q.shape[1] // (2 * n)
    yc, z, x, _, chunk = g.shape
    outs = (
        jax.ShapeDtypeStruct((rows, wide + 2 * DH), q.dtype),
        *(jax.ShapeDtypeStruct((rows, 2 * wide + 2 * DH), q.dtype),) * (n - 1),
        jax.ShapeDtypeStruct((yc, x, 1, z * chunk), g.dtype),
    )
    found = kernel_call(
        lambda *refs: pack_kernel(n, *refs),
        outs,
        (at, q, k, v, g),
        "pack",
        scratch=(pltpu.SemaphoreType.DMA((4 * n - 1 + z,)),),
        in_specs=[pl.BlockSpec(memory_space=pltpu.SMEM)] + [pl.BlockSpec(memory_space=pl.ANY)] * 4,
    )
    return found[:n], found[-1]


def stack_kernel(n, *refs):
    for hop in range(n):
        refs[n][hop] = refs[hop][:, -refs[n].shape[-1] :]


def stacked(pieces, wide):
    n, rows = len(pieces), pieces[0].shape[0]
    vmem = pl.BlockSpec(memory_space=pltpu.VMEM)
    return kernel_call(
        lambda *refs: stack_kernel(n, *refs),
        (jax.ShapeDtypeStruct((n, rows, wide), pieces[0].dtype),),
        tuple(pieces),
        "stack",
        in_specs=[vmem] * n,
    )[0]


def cut_kernel(n, at_ref, kv_ref, *to):
    _, x = place(at_ref, n)
    for hop in range(n):
        to[hop][...] = kv_ref[lax.div(lax.rem(x + hop, n), 2)]


def cut(at, kv, n):
    outs = (jax.ShapeDtypeStruct(kv.shape[1:], kv.dtype),) * n
    return kernel_call(lambda *refs: cut_kernel(n, *refs), outs, (at, kv), "cut")


def share_kernel(copies, parts_ref, to):
    total = jnp.sum(parts_ref[...], axis=0)
    chunk = to.shape[-1]
    for i in range(to.shape[0]):
        z = i % (to.shape[0] // copies)
        to[i] = total[:, z * chunk : (z + 1) * chunk]


def shared(parts, dp, z):
    chunk = parts.shape[-1] // z
    return kernel_call(
        lambda *refs: share_kernel(dp, *refs),
        (jax.ShapeDtypeStruct((dp * z, 1, chunk), parts.dtype),),
        (parts,),
        "share",
        in_specs=[pl.BlockSpec(memory_space=pltpu.VMEM)],
    )[0]


def gather_kernel(n, at_ref, *refs):
    near, far, (kv_ref, last_ref) = refs[:n], refs[n : 2 * n], refs[2 * n :]
    side, x = place(at_ref, n)
    rows, width = far[0].shape

    def put(half, chunk, value):
        kv_ref[pl.ds(pl.multiple_of((half * n + chunk) * rows, rows), rows)] = value

    for hop in range(n):
        chunk = lax.rem(x + n - hop, n)
        wide = near[0].shape[1] - width
        put(side, chunk, near[hop][:, wide : wide + width])
        put(1 - side, chunk, far[hop][...])
    last_ref[...] = kv_ref[kv_ref.shape[0] - last_ref.shape[0] :]


def gathered(at, near, far, reach):
    rows, width = far[0].shape
    n = len(near)
    outs = (
        jax.ShapeDtypeStruct((2 * n * rows, width), jnp.bfloat16),
        jax.ShapeDtypeStruct((reach, width), jnp.bfloat16),
    )
    return kernel_call(lambda *refs: gather_kernel(n, *refs), outs, (at, *near, *far), "gather")


def attend_kernel(n, is_near, count, at_ref, kv_ref, prior_ref, *refs):
    pieces, out_ref, q_s, older_s, out_s, sem = refs[:count], *refs[-5:]
    side, x = place(at_ref, n)
    half = side if is_near else 1 - side
    rows, wide = q_s.shape[0] // n, q_s.shape[1]
    reach = prior_ref.shape[0]
    for hop in range(n):
        chunk = lax.rem(x + n - hop, n)
        value = pieces[hop][:, :wide] if is_near else pieces[0][hop - 1] if hop else pieces[1][n // 2]
        q_s[pl.ds(pl.multiple_of(chunk * rows, rows), rows)] = value
    start = pl.multiple_of(half * n * rows, reach)

    @pl.when(half == 0)
    def _():
        older_s[...] = prior_ref[...]

    @pl.when(half != 0)
    def _():
        older_s[...] = kv_ref[n * rows - reach : n * rows]

    row = lax.broadcasted_iota(jnp.int32, (reach, reach), 0)
    col = lax.broadcasted_iota(jnp.int32, (reach, reach), 1)
    newer = col <= row
    across = (((1,), (1,)), ((), ()))
    for block in range(n * rows // reach):
        here = pl.ds(block * reach, reach)
        now = pl.ds(pl.multiple_of(start + block * reach, reach), reach)
        if block:
            older_ref, older = kv_ref, pl.ds(pl.multiple_of(start + (block - 1) * reach, reach), reach)
        else:
            older_ref, older = older_s, slice(None)
        for head in range(wide // DH):
            lanes = pl.ds(head * DH, DH)
            q = q_s[here, lanes]
            old = lax.dot_general(q, older_ref[older, :DH], across, preferred_element_type=jnp.float32)
            new = lax.dot_general(q, kv_ref[now, :DH], across, preferred_element_type=jnp.float32)
            scores = jnp.where(newer, new, old) * DH**-0.5
            expo = jnp.exp(scores - jnp.max(scores, axis=-1, keepdims=True))
            weights = (expo / jnp.sum(expo, axis=-1, keepdims=True)).astype(jnp.bfloat16)
            none = jnp.zeros_like(weights)
            out = jnp.dot(
                jnp.where(newer, weights, none), kv_ref[now, DH:], preferred_element_type=jnp.float32
            ) + jnp.dot(
                jnp.where(newer, none, weights), older_ref[older, DH:], preferred_element_type=jnp.float32
            )
            out_s[here, lanes] = out.astype(jnp.bfloat16)
    copy = pltpu.make_async_copy(out_s, out_ref.at[pl.ds(start, n * rows)], sem)
    copy.start()
    copy.wait()


def attended_half(at, kv, prior, pieces, n, wide, onto=None):
    reach, total = prior.shape[0], kv.shape[0]
    vmem, somewhere = pl.BlockSpec(memory_space=pltpu.VMEM), pl.BlockSpec(memory_space=pl.ANY)
    is_near = onto is None
    ins = (at, kv, prior, *pieces) + (() if is_near else (onto,))
    return kernel_call(
        lambda *refs: attend_kernel(n, is_near, len(pieces), *refs),
        (jax.ShapeDtypeStruct((total, wide), jnp.bfloat16),),
        ins,
        "attend",
        scratch=(
            pltpu.VMEM((total // 2, wide), jnp.bfloat16),
            pltpu.VMEM(prior.shape, jnp.bfloat16),
            pltpu.VMEM((total // 2, wide), jnp.bfloat16),
            pltpu.SemaphoreType.DMA,
        ),
        limit=16 << 20,
        in_specs=[pl.BlockSpec(memory_space=pltpu.SMEM)]
        + [vmem] * (2 + len(pieces))
        + ([] if is_near else [somewhere]),
        out_specs=(somewhere,),
        input_output_aliases={} if is_near else {3 + len(pieces): 0},
        cost_estimate=pl.CostEstimate(
            flops=4 * total * wide * reach, bytes_accessed=2 * total * wide * 2, transcendentals=total * reach
        ),
    )[0]


def step(queries, keys, values, grad_parts):
    dp, y, c, z, n = (lax.axis_size(a) for a in ("dp", *BLK_AA))
    at = lax.axis_index(AA).astype(jnp.int32).reshape(1)
    wide = queries.shape[2] // (z * n)
    reach = queries.shape[1] * 2
    chunks = grad_parts.reshape(y * c, z, n, 1, -1)
    kv_far = packed_far(at, queries[0], keys[0], values[0], n)
    sent, parts = packed(at, queries[0], keys[0], values[0], chunks, n)

    def along_x(value, hop):
        return lax.ppermute(value, "aa_1", [(x, (x + hop) % n) for x in range(n)])

    def across_z(value):
        return lax.ppermute(value, "aa_0", [(s, 1 - s) for s in range(z)])

    kv_far = across_z(kv_far)
    near = [sent[0]] + [along_x(sent[hop], hop) for hop in range(1, n)]
    parts = parts.reshape(y * c * n, 1, -1)
    parts = lax.all_to_all(parts, ("blk_0", "blk_1", "aa_1"), 0, 0, tiled=True)
    q_far = stacked(near[1:], wide)
    q_far = across_z(q_far)
    far = cut(at, kv_far, n)
    far = [far[0]] + [along_x(far[hop], hop) for hop in range(1, n)]
    kv, last = gathered(at, near, far, reach)
    prior = lax.ppermute(last, BLK, [(i, i + 1) for i in range(y * c - 1)])
    rows = attended_half(at, kv, prior, near, n, wide)

    share = shared(parts, dp, z)
    share = lax.all_to_all(share, ("dp", "aa_0"), 0, 0, tiled=True)
    grad_mean = jnp.sum(share, axis=(0, 1)) / (dp * y * c * z * n)

    rows = attended_half(at, kv, prior, (q_far, kv_far), n, wide, rows)
    return rows[None], grad_mean


def solution(mesh):
    torus = Mesh(
        mesh.devices.reshape(mesh.shape["dp"], 8, 2, 2, 4), ("dp", "blk_0", "blk_1", "aa_0", "aa_1")
    )
    placed = P("dp", BLK_AA, None)
    return jax.shard_map(
        step,
        mesh=torus,
        in_specs=(placed,) * 4,
        out_specs=(P("dp", BLK, AA), P(BLK_AA)),
        check_vma=False,
    )
```

```python
import jax
import jax.numpy as jnp
from jax import lax
from jax.experimental import pallas as pl
from jax.experimental.pallas import tpu as pltpu
from jax.sharding import Mesh
from jax.sharding import PartitionSpec as P

DH = 128
BLK = ("blk_0", "blk_1")
AA = ("aa_0", "aa_1")
BLK_AA = ("blk_0", "blk_1", "aa_0", "aa_1")


def place(at_ref, n):
    at = at_ref[0]
    return lax.div(at, n), lax.rem(at, n)


def place(at_ref, n):
    at = at_ref[0]
    return lax.div(at, n), lax.rem(at, n)


def run_all(moves, sems):
    copies = [pltpu.make_async_copy(a, b, sems.at[i]) for i, (a, b) in enumerate(moves)]
    for copy in copies:
        copy.start()
    for copy in copies:
        copy.wait()


def lanes_of(ref, index, width):
    return ref.at[:, pl.ds(pl.multiple_of(index * width, width), width)]


def pack_far_kernel(n, at_ref, q_ref, k_ref, v_ref, kv_to, sems):
    side, x = place(at_ref, n)
    moves = [(lanes_of(q_ref, (1 - side) * n + x, 2 * DH), kv_to.at[n // 2])]
    for i in range(n // 2):
        head = (1 - side) * (n // 2) + i
        moves.append((lanes_of(k_ref, head, DH), kv_to.at[i, :, :DH]))
        moves.append((lanes_of(v_ref, head, DH), kv_to.at[i, :, DH:]))
    run_all(moves, sems)


def pack_parts_kernel(g_ref, g_to, sems):
    chunk = g_ref.shape[-1]
    moves = [(g_ref.at[:, z], g_to.at[:, :, :, z * chunk : (z + 1) * chunk]) for z in range(g_ref.shape[1])]
    run_all(moves, sems)


def pack_kernel(n, at_ref, q_ref, k_ref, v_ref, *refs):
    to, sems = refs[:n], refs[n]
    side, x = place(at_ref, n)
    wide = q_ref.shape[1] // (2 * n)
    moves = []
    for hop in range(n):
        target = lax.rem(x + hop, n)
        head = side * (n // 2) + lax.div(target, 2)
        moves.append((lanes_of(q_ref, side * n + target, wide), to[hop].at[:, :wide]))
        moves.append((lanes_of(k_ref, head, DH), to[hop].at[:, wide : wide + DH]))
        moves.append((lanes_of(v_ref, head, DH), to[hop].at[:, wide + DH : wide + 2 * DH]))
        if hop:
            moves.append((lanes_of(q_ref, (1 - side) * n + target, wide), to[hop].at[:, wide + 2 * DH :]))
    run_all(moves, sems)


def kernel_call(body, outs, ins, name, scratch=(), limit=8 << 20, **more):
    vmem = pl.BlockSpec(memory_space=pltpu.VMEM)
    settings = dict(
        out_shape=outs,
        in_specs=[pl.BlockSpec(memory_space=pltpu.SMEM)] + [vmem] * (len(ins) - 1),
        out_specs=(vmem,) * len(outs),
        scratch_shapes=list(scratch),
        compiler_params=pltpu.CompilerParams(vmem_limit_bytes=limit),
        name=name,
    )
    settings.update(more)
    return pl.pallas_call(body, **settings)(*ins)


def packed_far(at, q, k, v, n):
    return kernel_call(
        lambda *refs: pack_far_kernel(n, *refs),
        (jax.ShapeDtypeStruct((n // 2 + 1, k.shape[0], 2 * DH), k.dtype),),
        (at, q, k, v),
        "pack_far",
        limit=60 << 20,
        scratch=(pltpu.SemaphoreType.DMA((n + 1,)),),
        in_specs=[pl.BlockSpec(memory_space=pltpu.SMEM)] + [pl.BlockSpec(memory_space=pl.ANY)] * 3,
    )[0]


def packed(at, q, k, v, n):
    rows, wide = q.shape[0], q.shape[1] // (2 * n)
    outs = (
        jax.ShapeDtypeStruct((rows, wide + 2 * DH), q.dtype),
        *(jax.ShapeDtypeStruct((rows, 2 * wide + 2 * DH), q.dtype),) * (n - 1),
    )
    return kernel_call(
        lambda *refs: pack_kernel(n, *refs),
        outs,
        (at, q, k, v),
        "pack",
        scratch=(pltpu.SemaphoreType.DMA((4 * n - 1,)),),
        in_specs=[pl.BlockSpec(memory_space=pltpu.SMEM)] + [pl.BlockSpec(memory_space=pl.ANY)] * 3,
    )


def packed_parts(g):
    yc, z, x, _, chunk = g.shape
    return kernel_call(
        pack_parts_kernel,
        (jax.ShapeDtypeStruct((yc, x, 1, z * chunk), g.dtype),),
        (g,),
        "pack_parts",
        scratch=(pltpu.SemaphoreType.DMA((z,)),),
        in_specs=[pl.BlockSpec(memory_space=pl.ANY)],
    )[0]


def stack_kernel(n, *refs):
    for hop in range(n):
        refs[n][hop] = refs[hop][:, -refs[n].shape[-1] :]


def stacked(pieces, wide):
    n, rows = len(pieces), pieces[0].shape[0]
    vmem = pl.BlockSpec(memory_space=pltpu.VMEM)
    return kernel_call(
        lambda *refs: stack_kernel(n, *refs),
        (jax.ShapeDtypeStruct((n, rows, wide), pieces[0].dtype),),
        tuple(pieces),
        "stack",
        in_specs=[vmem] * n,
    )[0]


def cut_kernel(n, at_ref, kv_ref, *to):
    _, x = place(at_ref, n)
    for hop in range(n):
        to[hop][...] = kv_ref[lax.div(lax.rem(x + hop, n), 2)]


def cut(at, kv, n):
    outs = (jax.ShapeDtypeStruct(kv.shape[1:], kv.dtype),) * n
    return kernel_call(lambda *refs: cut_kernel(n, *refs), outs, (at, kv), "cut")


def share_kernel(copies, parts_ref, to):
    total = jnp.sum(parts_ref[...], axis=0)
    chunk = to.shape[-1]
    for i in range(to.shape[0]):
        z = i % (to.shape[0] // copies)
        to[i] = total[:, z * chunk : (z + 1) * chunk]


def shared(parts, dp, z):
    chunk = parts.shape[-1] // z
    return kernel_call(
        lambda *refs: share_kernel(dp, *refs),
        (jax.ShapeDtypeStruct((dp * z, 1, chunk), parts.dtype),),
        (parts,),
        "share",
        in_specs=[pl.BlockSpec(memory_space=pltpu.VMEM)],
    )[0]


def mean_kernel(count, share_ref, to):
    to[...] = jnp.sum(share_ref[...], axis=0) / count


def averaged(share, count):
    return kernel_call(
        lambda *refs: mean_kernel(count, *refs),
        (jax.ShapeDtypeStruct(share.shape[1:], share.dtype),),
        (share,),
        "mean",
        in_specs=[pl.BlockSpec(memory_space=pltpu.VMEM)],
    )[0].reshape(-1)


def gather_kernel(n, at_ref, *refs):
    near, far, (kv_ref, last_ref) = refs[:n], refs[n : 2 * n], refs[2 * n :]
    side, x = place(at_ref, n)
    rows, width = far[0].shape

    def put(half, chunk, value):
        kv_ref[pl.ds(pl.multiple_of((half * n + chunk) * rows, rows), rows)] = value

    for hop in range(n):
        chunk = lax.rem(x + n - hop, n)
        wide = near[0].shape[1] - width
        put(side, chunk, near[hop][:, wide : wide + width])
        put(1 - side, chunk, far[hop][...])
    last_ref[...] = kv_ref[kv_ref.shape[0] - last_ref.shape[0] :]


def gathered(at, near, far, reach):
    rows, width = far[0].shape
    n = len(near)
    outs = (
        jax.ShapeDtypeStruct((2 * n * rows, width), jnp.bfloat16),
        jax.ShapeDtypeStruct((reach, width), jnp.bfloat16),
    )
    return kernel_call(lambda *refs: gather_kernel(n, *refs), outs, (at, *near, *far), "gather")


def attend_kernel(n, is_near, count, at_ref, kv_ref, prior_ref, *refs):
    pieces, out_ref, q_s, older_s, out_s, sem = refs[:count], *refs[-5:]
    side, x = place(at_ref, n)
    half = side if is_near else 1 - side
    rows, wide = q_s.shape[0] // n, q_s.shape[1]
    reach = prior_ref.shape[0]
    for hop in range(n):
        chunk = lax.rem(x + n - hop, n)
        value = pieces[hop][:, :wide] if is_near else pieces[0][hop - 1] if hop else pieces[1][n // 2]
        q_s[pl.ds(pl.multiple_of(chunk * rows, rows), rows)] = value
    start = pl.multiple_of(half * n * rows, reach)

    @pl.when(half == 0)
    def _():
        older_s[...] = prior_ref[...]

    @pl.when(half != 0)
    def _():
        older_s[...] = kv_ref[n * rows - reach : n * rows]

    row = lax.broadcasted_iota(jnp.int32, (reach, reach), 0)
    col = lax.broadcasted_iota(jnp.int32, (reach, reach), 1)
    newer = col <= row
    across = (((1,), (1,)), ((), ()))
    for block in range(n * rows // reach):
        here = pl.ds(block * reach, reach)
        now = pl.ds(pl.multiple_of(start + block * reach, reach), reach)
        if block:
            older_ref, older = kv_ref, pl.ds(pl.multiple_of(start + (block - 1) * reach, reach), reach)
        else:
            older_ref, older = older_s, slice(None)
        for head in range(wide // DH):
            lanes = pl.ds(head * DH, DH)
            q = q_s[here, lanes]
            old = lax.dot_general(q, older_ref[older, :DH], across, preferred_element_type=jnp.float32)
            new = lax.dot_general(q, kv_ref[now, :DH], across, preferred_element_type=jnp.float32)
            scores = jnp.where(newer, new, old) * DH**-0.5
            expo = jnp.exp(scores - jnp.max(scores, axis=-1, keepdims=True))
            weights = (expo / jnp.sum(expo, axis=-1, keepdims=True)).astype(jnp.bfloat16)
            none = jnp.zeros_like(weights)
            out = jnp.dot(
                jnp.where(newer, weights, none), kv_ref[now, DH:], preferred_element_type=jnp.float32
            ) + jnp.dot(
                jnp.where(newer, none, weights), older_ref[older, DH:], preferred_element_type=jnp.float32
            )
            out_s[here, lanes] = out.astype(jnp.bfloat16)
    copy = pltpu.make_async_copy(out_s, out_ref.at[pl.ds(start, n * rows)], sem)
    copy.start()
    copy.wait()


def attended_half(at, kv, prior, pieces, n, wide, onto=None):
    reach, total = prior.shape[0], kv.shape[0]
    vmem, somewhere = pl.BlockSpec(memory_space=pltpu.VMEM), pl.BlockSpec(memory_space=pl.ANY)
    is_near = onto is None
    ins = (at, kv, prior, *pieces) + (() if is_near else (onto,))
    return kernel_call(
        lambda *refs: attend_kernel(n, is_near, len(pieces), *refs),
        (jax.ShapeDtypeStruct((total, wide), jnp.bfloat16),),
        ins,
        "attend",
        scratch=(
            pltpu.VMEM((total // 2, wide), jnp.bfloat16),
            pltpu.VMEM(prior.shape, jnp.bfloat16),
            pltpu.VMEM((total // 2, wide), jnp.bfloat16),
            pltpu.SemaphoreType.DMA,
        ),
        limit=16 << 20,
        in_specs=[pl.BlockSpec(memory_space=pltpu.SMEM)]
        + [vmem] * (2 + len(pieces))
        + ([] if is_near else [somewhere]),
        out_specs=(somewhere,),
        input_output_aliases={} if is_near else {3 + len(pieces): 0},
        cost_estimate=pl.CostEstimate(
            flops=4 * total * wide * reach, bytes_accessed=2 * total * wide * 2, transcendentals=total * reach
        ),
    )[0]


def step(queries, keys, values, grad_parts):
    dp, y, c, z, n = (lax.axis_size(a) for a in ("dp", *BLK_AA))
    at = lax.axis_index(AA).astype(jnp.int32).reshape(1)
    wide = queries.shape[2] // (z * n)
    reach = queries.shape[1] * 2
    chunks = grad_parts.reshape(y * c, z, n, 1, -1)
    kv_far = packed_far(at, queries[0], keys[0], values[0], n)
    sent = packed(at, queries[0], keys[0], values[0], n)
    parts = packed_parts(chunks)

    def along_x(value, hop):
        return lax.ppermute(value, "aa_1", [(x, (x + hop) % n) for x in range(n)])

    def across_z(value):
        return lax.ppermute(value, "aa_0", [(s, 1 - s) for s in range(z)])

    kv_far = across_z(kv_far)
    near = [sent[0]] + [along_x(sent[hop], hop) for hop in range(1, n)]
    parts = parts.reshape(y * c * n, 1, -1)
    parts = lax.all_to_all(parts, ("blk_0", "blk_1", "aa_1"), 0, 0, tiled=True)
    q_far = stacked(near[1:], wide)
    q_far = across_z(q_far)
    far = cut(at, kv_far, n)
    far = [far[0]] + [along_x(far[hop], hop) for hop in range(1, n)]
    kv, last = gathered(at, near, far, reach)
    prior = lax.ppermute(last, BLK, [(i, i + 1) for i in range(y * c - 1)])
    rows = attended_half(at, kv, prior, near, n, wide)

    share = shared(parts, dp, z)
    share = lax.all_to_all(share, ("dp", "aa_0"), 0, 0, tiled=True)
    grad_mean = averaged(share, dp * y * c * z * n)

    rows = attended_half(at, kv, prior, (q_far, kv_far), n, wide, rows)
    return rows[None], grad_mean


def solution(mesh):
    torus = Mesh(
        mesh.devices.reshape(mesh.shape["dp"], 8, 2, 2, 4), ("dp", "blk_0", "blk_1", "aa_0", "aa_1")
    )
    placed = P("dp", BLK_AA, None)
    return jax.shard_map(
        step,
        mesh=torus,
        in_specs=(placed,) * 4,
        out_specs=(P("dp", BLK, AA), P(BLK_AA)),
        check_vma=False,
    )
```

```python
import jax
import jax.numpy as jnp
from jax import lax
from jax.experimental import pallas as pl
from jax.experimental.pallas import tpu as pltpu
from jax.sharding import Mesh
from jax.sharding import PartitionSpec as P

DH = 128
BLK = ("blk_0", "blk_1")
AA = ("aa_0", "aa_1")
BLK_AA = ("blk_0", "blk_1", "aa_0", "aa_1")


def place(at_ref, n):
    at = at_ref[0]
    return lax.div(at, n), lax.rem(at, n)


def place(at_ref, n):
    at = at_ref[0]
    return lax.div(at, n), lax.rem(at, n)


def run_all(moves, sems):
    copies = [pltpu.make_async_copy(a, b, sems.at[i]) for i, (a, b) in enumerate(moves)]
    for copy in copies:
        copy.start()
    for copy in copies:
        copy.wait()


def lanes_of(ref, index, width):
    return ref.at[:, pl.ds(pl.multiple_of(index * width, width), width)]


def pack_far_kernel(n, at_ref, q_ref, k_ref, v_ref, kv_to, sems):
    side, x = place(at_ref, n)
    moves = [(lanes_of(q_ref, (1 - side) * n + x, 2 * DH), kv_to.at[n // 2])]
    for i in range(n // 2):
        head = (1 - side) * (n // 2) + i
        moves.append((lanes_of(k_ref, head, DH), kv_to.at[i, :, :DH]))
        moves.append((lanes_of(v_ref, head, DH), kv_to.at[i, :, DH:]))
    run_all(moves, sems)


def pack_parts_kernel(core_ref, g_ref, own, other, sems):
    core, chunk = core_ref[0], g_ref.shape[-1]
    moves = []
    for z in range(g_ref.shape[2]):
        lanes = slice(z * chunk, (z + 1) * chunk)
        moves.append((g_ref.at[:, core, z], own.at[:, :, :, lanes]))
        moves.append((g_ref.at[:, 1 - core, z], other.at[:, :, :, lanes]))
    run_all(moves, sems)


def add_kernel(a_ref, b_ref, to):
    to[...] = a_ref[...] + b_ref[...]


def added(a, b):
    vmem = pl.BlockSpec(memory_space=pltpu.VMEM)
    outs = (jax.ShapeDtypeStruct(a.shape, a.dtype),)
    return kernel_call(add_kernel, outs, (a, b), "add", in_specs=[vmem, vmem])[0]


def pack_kernel(n, at_ref, q_ref, k_ref, v_ref, *refs):
    to, sems = refs[:n], refs[n]
    side, x = place(at_ref, n)
    wide = q_ref.shape[1] // (2 * n)
    moves = []
    for hop in range(n):
        target = lax.rem(x + hop, n)
        head = side * (n // 2) + lax.div(target, 2)
        moves.append((lanes_of(q_ref, side * n + target, wide), to[hop].at[:, :wide]))
        moves.append((lanes_of(k_ref, head, DH), to[hop].at[:, wide : wide + DH]))
        moves.append((lanes_of(v_ref, head, DH), to[hop].at[:, wide + DH : wide + 2 * DH]))
        if hop:
            moves.append((lanes_of(q_ref, (1 - side) * n + target, wide), to[hop].at[:, wide + 2 * DH :]))
    run_all(moves, sems)


def kernel_call(body, outs, ins, name, scratch=(), limit=8 << 20, **more):
    vmem = pl.BlockSpec(memory_space=pltpu.VMEM)
    settings = dict(
        out_shape=outs,
        in_specs=[pl.BlockSpec(memory_space=pltpu.SMEM)] + [vmem] * (len(ins) - 1),
        out_specs=(vmem,) * len(outs),
        scratch_shapes=list(scratch),
        compiler_params=pltpu.CompilerParams(vmem_limit_bytes=limit),
        name=name,
    )
    settings.update(more)
    return pl.pallas_call(body, **settings)(*ins)


def packed_far(at, q, k, v, n):
    return kernel_call(
        lambda *refs: pack_far_kernel(n, *refs),
        (jax.ShapeDtypeStruct((n // 2 + 1, k.shape[0], 2 * DH), k.dtype),),
        (at, q, k, v),
        "pack_far",
        limit=60 << 20,
        scratch=(pltpu.SemaphoreType.DMA((n + 1,)),),
        in_specs=[pl.BlockSpec(memory_space=pltpu.SMEM)] + [pl.BlockSpec(memory_space=pl.ANY)] * 3,
    )[0]


def packed(at, q, k, v, n):
    rows, wide = q.shape[0], q.shape[1] // (2 * n)
    outs = (
        jax.ShapeDtypeStruct((rows, wide + 2 * DH), q.dtype),
        *(jax.ShapeDtypeStruct((rows, 2 * wide + 2 * DH), q.dtype),) * (n - 1),
    )
    return kernel_call(
        lambda *refs: pack_kernel(n, *refs),
        outs,
        (at, q, k, v),
        "pack",
        scratch=(pltpu.SemaphoreType.DMA((4 * n - 1,)),),
        in_specs=[pl.BlockSpec(memory_space=pltpu.SMEM)] + [pl.BlockSpec(memory_space=pl.ANY)] * 3,
    )


def packed_parts(core, g):
    y, _, z, x, _, chunk = g.shape
    return kernel_call(
        pack_parts_kernel,
        (jax.ShapeDtypeStruct((y, x, 1, z * chunk), g.dtype),) * 2,
        (core, g),
        "pack_parts",
        scratch=(pltpu.SemaphoreType.DMA((2 * z,)),),
        in_specs=[pl.BlockSpec(memory_space=pltpu.SMEM), pl.BlockSpec(memory_space=pl.ANY)],
    )


def stack_kernel(n, *refs):
    for hop in range(n):
        refs[n][hop] = refs[hop][:, -refs[n].shape[-1] :]


def stacked(pieces, wide):
    n, rows = len(pieces), pieces[0].shape[0]
    vmem = pl.BlockSpec(memory_space=pltpu.VMEM)
    return kernel_call(
        lambda *refs: stack_kernel(n, *refs),
        (jax.ShapeDtypeStruct((n, rows, wide), pieces[0].dtype),),
        tuple(pieces),
        "stack",
        in_specs=[vmem] * n,
    )[0]


def cut_kernel(n, at_ref, kv_ref, *to):
    _, x = place(at_ref, n)
    for hop in range(n):
        to[hop][...] = kv_ref[lax.div(lax.rem(x + hop, n), 2)]


def cut(at, kv, n):
    outs = (jax.ShapeDtypeStruct(kv.shape[1:], kv.dtype),) * n
    return kernel_call(lambda *refs: cut_kernel(n, *refs), outs, (at, kv), "cut")


def share_kernel(copies, parts_ref, to):
    total = jnp.sum(parts_ref[...], axis=0)
    chunk = to.shape[-1]
    for i in range(to.shape[0]):
        z = i % (to.shape[0] // copies)
        to[i] = total[:, z * chunk : (z + 1) * chunk]


def shared(parts, dp, z):
    chunk = parts.shape[-1] // z
    return kernel_call(
        lambda *refs: share_kernel(dp, *refs),
        (jax.ShapeDtypeStruct((dp * z, 1, chunk), parts.dtype),),
        (parts,),
        "share",
        in_specs=[pl.BlockSpec(memory_space=pltpu.VMEM)],
    )[0]


def mean_kernel(count, share_ref, to):
    to[...] = jnp.sum(share_ref[...], axis=0) / count


def averaged(share, count):
    return kernel_call(
        lambda *refs: mean_kernel(count, *refs),
        (jax.ShapeDtypeStruct(share.shape[1:], share.dtype),),
        (share,),
        "mean",
        in_specs=[pl.BlockSpec(memory_space=pltpu.VMEM)],
    )[0].reshape(-1)


def gather_kernel(n, at_ref, *refs):
    near, far, (kv_ref, last_ref) = refs[:n], refs[n : 2 * n], refs[2 * n :]
    side, x = place(at_ref, n)
    rows, width = far[0].shape

    def put(half, chunk, value):
        kv_ref[pl.ds(pl.multiple_of((half * n + chunk) * rows, rows), rows)] = value

    for hop in range(n):
        chunk = lax.rem(x + n - hop, n)
        wide = near[0].shape[1] - width
        put(side, chunk, near[hop][:, wide : wide + width])
        put(1 - side, chunk, far[hop][...])
    last_ref[...] = kv_ref[kv_ref.shape[0] - last_ref.shape[0] :]


def gathered(at, near, far, reach):
    rows, width = far[0].shape
    n = len(near)
    outs = (
        jax.ShapeDtypeStruct((2 * n * rows, width), jnp.bfloat16),
        jax.ShapeDtypeStruct((reach, width), jnp.bfloat16),
    )
    return kernel_call(lambda *refs: gather_kernel(n, *refs), outs, (at, *near, *far), "gather")


def attend_kernel(n, is_near, count, at_ref, kv_ref, prior_ref, *refs):
    pieces, out_ref, q_s, older_s, out_s, sem = refs[:count], *refs[-5:]
    side, x = place(at_ref, n)
    half = side if is_near else 1 - side
    rows, wide = q_s.shape[0] // n, q_s.shape[1]
    reach = prior_ref.shape[0]
    for hop in range(n):
        chunk = lax.rem(x + n - hop, n)
        value = pieces[hop][:, :wide] if is_near else pieces[0][hop - 1] if hop else pieces[1][n // 2]
        q_s[pl.ds(pl.multiple_of(chunk * rows, rows), rows)] = value
    start = pl.multiple_of(half * n * rows, reach)

    @pl.when(half == 0)
    def _():
        older_s[...] = prior_ref[...]

    @pl.when(half != 0)
    def _():
        older_s[...] = kv_ref[n * rows - reach : n * rows]

    row = lax.broadcasted_iota(jnp.int32, (reach, reach), 0)
    col = lax.broadcasted_iota(jnp.int32, (reach, reach), 1)
    newer = col <= row
    across = (((1,), (1,)), ((), ()))
    for block in range(n * rows // reach):
        here = pl.ds(block * reach, reach)
        now = pl.ds(pl.multiple_of(start + block * reach, reach), reach)
        if block:
            older_ref, older = kv_ref, pl.ds(pl.multiple_of(start + (block - 1) * reach, reach), reach)
        else:
            older_ref, older = older_s, slice(None)
        for head in range(wide // DH):
            lanes = pl.ds(head * DH, DH)
            q = q_s[here, lanes]
            old = lax.dot_general(q, older_ref[older, :DH], across, preferred_element_type=jnp.float32)
            new = lax.dot_general(q, kv_ref[now, :DH], across, preferred_element_type=jnp.float32)
            scores = jnp.where(newer, new, old) * DH**-0.5
            expo = jnp.exp(scores - jnp.max(scores, axis=-1, keepdims=True))
            weights = (expo / jnp.sum(expo, axis=-1, keepdims=True)).astype(jnp.bfloat16)
            none = jnp.zeros_like(weights)
            out = jnp.dot(
                jnp.where(newer, weights, none), kv_ref[now, DH:], preferred_element_type=jnp.float32
            ) + jnp.dot(
                jnp.where(newer, none, weights), older_ref[older, DH:], preferred_element_type=jnp.float32
            )
            out_s[here, lanes] = out.astype(jnp.bfloat16)
    copy = pltpu.make_async_copy(out_s, out_ref.at[pl.ds(start, n * rows)], sem)
    copy.start()
    copy.wait()


def attended_half(at, kv, prior, pieces, n, wide, onto=None):
    reach, total = prior.shape[0], kv.shape[0]
    vmem, somewhere = pl.BlockSpec(memory_space=pltpu.VMEM), pl.BlockSpec(memory_space=pl.ANY)
    is_near = onto is None
    ins = (at, kv, prior, *pieces) + (() if is_near else (onto,))
    return kernel_call(
        lambda *refs: attend_kernel(n, is_near, len(pieces), *refs),
        (jax.ShapeDtypeStruct((total, wide), jnp.bfloat16),),
        ins,
        "attend",
        scratch=(
            pltpu.VMEM((total // 2, wide), jnp.bfloat16),
            pltpu.VMEM(prior.shape, jnp.bfloat16),
            pltpu.VMEM((total // 2, wide), jnp.bfloat16),
            pltpu.SemaphoreType.DMA,
        ),
        limit=16 << 20,
        in_specs=[pl.BlockSpec(memory_space=pltpu.SMEM)]
        + [vmem] * (2 + len(pieces))
        + ([] if is_near else [somewhere]),
        out_specs=(somewhere,),
        input_output_aliases={} if is_near else {3 + len(pieces): 0},
        cost_estimate=pl.CostEstimate(
            flops=4 * total * wide * reach, bytes_accessed=2 * total * wide * 2, transcendentals=total * reach
        ),
    )[0]


def step(queries, keys, values, grad_parts):
    dp, y, c, z, n = (lax.axis_size(a) for a in ("dp", *BLK_AA))
    at = lax.axis_index(AA).astype(jnp.int32).reshape(1)
    wide = queries.shape[2] // (z * n)
    reach = queries.shape[1] * 2
    chunks = grad_parts.reshape(y, c, z, n, 1, -1)
    core = lax.axis_index("blk_1").astype(jnp.int32).reshape(1)
    kv_far = packed_far(at, queries[0], keys[0], values[0], n)
    sent = packed(at, queries[0], keys[0], values[0], n)
    parts, parts_out = packed_parts(core, chunks)

    def along_x(value, hop):
        return lax.ppermute(value, "aa_1", [(x, (x + hop) % n) for x in range(n)])

    def across_z(value):
        return lax.ppermute(value, "aa_0", [(s, 1 - s) for s in range(z)])

    kv_far = across_z(kv_far)
    parts_in = lax.ppermute(parts_out, "blk_1", [(i, 1 - i) for i in range(c)])
    near = [sent[0]] + [along_x(sent[hop], hop) for hop in range(1, n)]
    parts = added(parts, parts_in)
    parts = parts.reshape(y * n, 1, -1)
    parts = lax.all_to_all(parts, ("blk_0", "aa_1"), 0, 0, tiled=True)
    q_far = stacked(near[1:], wide)
    q_far = across_z(q_far)
    far = cut(at, kv_far, n)
    far = [far[0]] + [along_x(far[hop], hop) for hop in range(1, n)]
    kv, last = gathered(at, near, far, reach)
    prior = lax.ppermute(last, BLK, [(i, i + 1) for i in range(y * c - 1)])
    rows = attended_half(at, kv, prior, near, n, wide)

    share = shared(parts, dp, z)
    share = lax.all_to_all(share, ("dp", "aa_0"), 0, 0, tiled=True)
    grad_mean = averaged(share, dp * y * c * z * n)

    rows = attended_half(at, kv, prior, (q_far, kv_far), n, wide, rows)
    return rows[None], grad_mean


def solution(mesh):
    torus = Mesh(
        mesh.devices.reshape(mesh.shape["dp"], 8, 2, 2, 4), ("dp", "blk_0", "blk_1", "aa_0", "aa_1")
    )
    placed = P("dp", BLK_AA, None)
    return jax.shard_map(
        step,
        mesh=torus,
        in_specs=(placed,) * 4,
        out_specs=(P("dp", BLK, AA), P(BLK_AA)),
        check_vma=False,
    )
```
